256 devices in a mesh: group: 4 (over x, y), lat: 64 (over z, core).
Axes of the slice: x: 2, y: 2, z: 32, core: 2. Of those that a mesh axis runs over, the one named last changes fastest.
The devices are a block of a 4x8x32 slice.
Arguments:
- grid_values: bfloat16 [1792, 1440, 256], P(('group', 'lat')), parts along dimension 0, may hold values from -630 to 630
- lat_counts: int32 [64], replicated, may hold values from 1 to 7, 384 in all
- owner_wavenumber: int32 [384], replicated, may hold values from 0 to 383, each once
- legendre: bfloat16 [384, 384, 384], P('lat'), may hold values from -0.3125 to 0.3125
- quad_weight: float32 [384], replicated, may hold values from 0.3 to 3
- spectral_gain: float32 [384, 256], replicated, may hold values from 0.3 to 3
- channel_mix: bfloat16 [256, 256], replicated, may hold values from -0.375 to 0.375
Outputs:
- grid_output: bfloat16 [1792, 1440, 256], P(('group', 'lat')), parts along dimension 0
The draws below stay inside these ranges and needn't reach their ends.
There are 4 independent parts, one for each index of `group`. The reference program is written for one: setup_inputs(seed, part) draws one part's arguments, and reference() takes and returns one part's arrays. A program takes and returns all parts, laid end to end along the dimension named above; an argument that names none is the same for every part. Nothing has to cross between parts.
Inputs may be any that keep to these rules, and one draw needn't show every extreme that they name: `lat_counts`: some device has all 7 slots live. `owner_wavenumber`: each wavenumber appears once; device i of lat owns wavenumber slots i * 6 to (i + 1) * 6 - 1.
All inputs are finite; a program needn't handle non-finite values.
Results may differ from the reference program's by a relative error of at most 0.0095.
Values may be sent and summed in bfloat16 or wider, within the bound.
A program may use at most 64 MiB of HBM per device.

```python
import math
import jax
import jax.numpy as jnp
import numpy as np
from jax import lax

LONGITUDES = 1440
CHANNELS = 256
WAVES = 384
DEGREES = 384
LAT_SLOTS = 7
SLOTS_ALL = 448
LIVE_LATS = 384
N_LAT = 64


def draw_grid_values(key, part):
    key_rows = jax.random.fold_in(key, 11)
    key_scale = jax.random.fold_in(key, 12)
    key_mean = jax.random.fold_in(key, 13)
    key_noise = jax.random.fold_in(key, 14)
    position = jnp.arange(SLOTS_ALL, dtype=jnp.float32) / SLOTS_ALL
    jitter = jax.random.uniform(key_rows, (SLOTS_ALL,), minval=-0.1, maxval=0.1)
    row_scale = jnp.exp(jnp.log(10.0) * jnp.clip(position + jitter, 0.0, 1.0))
    chan_scale = jnp.exp(jax.random.uniform(key_scale, (CHANNELS,), minval=0.0, maxval=jnp.log(10.0)))
    chan_mean = jax.random.uniform(key_mean, (CHANNELS,), minval=-1.0, maxval=1.0)
    noise = jnp.clip(jax.random.normal(key_noise, (SLOTS_ALL, LONGITUDES, CHANNELS)), -6.0, 6.0)
    values = chan_mean[None, None, :] * chan_scale[None, None, :] + row_scale[:, None, None] * chan_scale[None, None, :] * noise
    return values.astype(jnp.float32).astype(jnp.bfloat16)


def block_levels(rng, shape, cuts, low, top_value):
    loudness, own = 1.0, jax.random.fold_in(rng, 6)
    for dim, blocks in cuts:
        heights = jnp.exp(jax.random.uniform(jax.random.fold_in(own, dim), (blocks,), jnp.float32, low / len(cuts), top_value / len(cuts)))
        loudness = loudness * jnp.repeat(heights, shape[dim] // blocks).reshape([-1 if axis == dim else 1 for axis in range(len(shape))])
    return loudness


def length_profile(number_of, total, reach, lean):
    weights = [(1 << 20) // math.isqrt(rank ** lean) + 1 for rank in range(2, number_of + 1)]
    spare, given = total - reach - (number_of - 1), [1] * (number_of - 1)
    while spare > 0:
        movable = [i for i in range(number_of - 1) if given[i] < reach]
        mass, budget = sum([weights[i] for i in movable]), spare
        for i in movable:
            extra = min(reach - given[i], max(1, budget * weights[i] // mass), spare)
            given[i] = given[i] + extra
            spare = spare - extra
    return np.array([reach] + given)


def ragged(key, amount, total, bound, slope):
    if amount == 2:
        one = jax.random.randint(key, (), max(1, total - bound), min(bound, total - 1) + 1)
        return jnp.stack([one, total - one])
    lengths = jnp.asarray(length_profile(amount, total, bound, slope), jnp.int32)
    pairs = (amount - 1) // 2
    giver, sink = lengths[1:1 + 2 * pairs:2], lengths[2:2 + 2 * pairs:2]
    room = jnp.minimum(giver - 1, bound - sink)
    shifted = jax.random.randint(jax.random.fold_in(key, 1), (pairs,), 0, 1 << 20) % (room + 1)
    lengths = lengths.at[1:1 + 2 * pairs:2].set(giver - shifted).at[2:2 + 2 * pairs:2].set(sink + shifted)
    return lengths[jax.random.permutation(jax.random.fold_in(key, 2), amount)]


def scatter_about(rng, extent, spread, limit, split=(), held_as=jnp.bfloat16):
    level = block_levels(rng, extent, split, -0.22, 0.18) if split else 1.0
    values = jax.random.normal(rng, extent, jnp.float32) * spread * level
    return jnp.minimum(jnp.maximum(values, -limit), limit).astype(held_as)


def setup_inputs(seed: int = 0, part: int = 0) -> dict:
    splits = jax.random.split(jax.random.key(seed), 8)
    own_keys = jax.random.split(jax.random.fold_in(splits[7], part), 8)
    return {
        "grid_values": draw_grid_values(jax.random.fold_in(jax.random.fold_in(splits[7], part), 71), part),
        "lat_counts": ragged(splits[1], N_LAT, LIVE_LATS, LAT_SLOTS, 2).astype(jnp.int32),
        "owner_wavenumber": jax.random.permutation(splits[2], WAVES).astype(jnp.int32),
        "legendre": scatter_about(splits[3], (WAVES, LIVE_LATS, DEGREES), LIVE_LATS ** -0.5, 0.3125, ((0, 64),)),
        "quad_weight": jnp.clip(jnp.exp(jax.random.uniform(splits[4], (LIVE_LATS,), jnp.float32, math.log(0.3), math.log(3.0))), 0.3, 3.0),
        "spectral_gain": jnp.clip(jnp.exp(jax.random.uniform(splits[5], (DEGREES, CHANNELS), jnp.float32, math.log(0.3), math.log(3.0))), 0.3, 3.0),
        "channel_mix": scatter_about(splits[6], (CHANNELS, CHANNELS), CHANNELS ** -0.5, 0.375),
    }


def live_slots(lat_counts, slot_count, live_total):
    devices = lat_counts.shape[0]
    starts = jnp.cumsum(lat_counts) - lat_counts
    device_ids = jnp.arange(devices, dtype=jnp.int32)
    slot_ids = jnp.arange(devices * slot_count, dtype=jnp.int32)
    holder = slot_ids // slot_count
    within = slot_ids - holder * slot_count
    holder_hot = holder[:, None] == device_ids[None, :]
    holder_count = lax.optimization_barrier(jnp.sum(jnp.where(holder_hot, lat_counts[None, :], 0), axis=1))
    holder_start = lax.optimization_barrier(jnp.sum(jnp.where(holder_hot, starts[None, :], 0), axis=1))
    slot_valid = within < holder_count
    slot_live = jnp.where(slot_valid, holder_start + within, 0).astype(jnp.int32)
    live_ids = jnp.arange(live_total, dtype=jnp.int32)
    reached = (starts[None, :] <= live_ids[:, None]).astype(jnp.int32)
    source = lax.optimization_barrier(jnp.sum(reached, axis=1)) - 1
    source_hot = source[:, None] == device_ids[None, :]
    source_start = lax.optimization_barrier(jnp.sum(jnp.where(source_hot, starts[None, :], 0), axis=1))
    live_slot = (source * slot_count + live_ids - source_start).astype(jnp.int32)
    return (slot_valid, slot_live, live_slot)

def wave_angles(wave_list, longitudes):
    points = jnp.arange(longitudes, dtype=jnp.int32)
    phase = wave_list[:, None] * points[None, :] % longitudes
    return phase.astype(jnp.float32) * (2.0 * math.pi / longitudes)

def forward_table(wave_list, longitudes):
    angle = wave_angles(wave_list, longitudes)
    factor = 1.0 / math.sqrt(longitudes)
    return jnp.stack([jnp.cos(angle) * factor, -jnp.sin(angle) * factor], axis=1).astype(jnp.bfloat16)

def inverse_table(wave_list, longitudes):
    angle = wave_angles(wave_list, longitudes)
    factor = 1.0 / math.sqrt(longitudes)
    doubled = jnp.where(wave_list > 0, 2.0, 1.0).astype(jnp.float32)[:, None] * factor
    return jnp.stack([jnp.cos(angle) * doubled, -jnp.sin(angle) * doubled], axis=1).astype(jnp.bfloat16)

def reference(grid_values, lat_counts, owner_wavenumber, legendre, quad_weight, spectral_gain, channel_mix):
    slot_valid, slot_live, live_slot = live_slots(lat_counts, LAT_SLOTS, LIVE_LATS)
    row_weight = slot_valid.astype(jnp.float32)[:, None, None]
    widened = grid_values.astype(jnp.float32) * row_weight
    points = LIVE_LATS * LONGITUDES
    channel_mean = lax.optimization_barrier(jnp.sum(widened, axis=(0, 1))) / points
    variance = lax.optimization_barrier(jnp.sum(widened * widened, axis=(0, 1))) / points - channel_mean * channel_mean
    normed = ((grid_values.astype(jnp.float32) - channel_mean) * lax.rsqrt(variance + 1e-05) * row_weight).astype(jnp.bfloat16)
    forward = forward_table(owner_wavenumber, LONGITUDES)
    spectra = jnp.einsum('skc,rtk->srtc', normed.astype(jnp.float32), forward.astype(jnp.float32)).astype(jnp.bfloat16)
    gathered = jnp.take(spectra, live_slot, axis=0)
    weighted = (gathered.astype(jnp.float32) * quad_weight[:, None, None, None]).astype(jnp.bfloat16)
    coefficient = jnp.einsum('rgl,grtc->rltc', legendre.astype(jnp.float32), weighted.astype(jnp.float32))
    degree_mask = (jnp.arange(DEGREES, dtype=jnp.int32)[None, :] >= owner_wavenumber[:, None]).astype(jnp.float32)
    filtered = (coefficient * degree_mask[:, :, None, None] * spectral_gain[None, :, None, :]).astype(jnp.bfloat16)
    mixed = jnp.dot(filtered.reshape(-1, CHANNELS), channel_mix, preferred_element_type=jnp.float32)
    mixed = mixed.astype(jnp.bfloat16).reshape(WAVES, DEGREES, 2, CHANNELS)
    synthesis = jnp.einsum('rgl,rltc->grtc', legendre.astype(jnp.float32), mixed.astype(jnp.float32)).astype(jnp.bfloat16)
    outgoing = jnp.where(slot_valid[:, None, None, None], jnp.take(synthesis, slot_live, axis=0), jnp.zeros((), jnp.bfloat16))
    inverse = inverse_table(owner_wavenumber, LONGITUDES)
    result = jnp.einsum('srtc,rtk->skc', outgoing.astype(jnp.float32), inverse.astype(jnp.float32))
    return result.astype(jnp.bfloat16)
```

```python
import functools
import math

import jax
import jax.numpy as jnp
import numpy as np
from jax import lax
from jax.experimental import pallas as pl
from jax.experimental.pallas import tpu as pltpu
from jax.sharding import PartitionSpec as P

MESH = pl.DeviceIdType.MESH
LANES = 128
PAIR = 2
ROWS = 8
BF16, F32 = jnp.bfloat16, jnp.float32


def dot(a, b, contract=(1, 0)):
    return lax.dot_general(
        a, b, (((contract[0],), (contract[1],)), ((), ())), preferred_element_type=F32
    )


def kernel(
    dims,
    counts,
    owner,
    x_hbm,
    leg_hbm,
    coef,
    cos_b,
    sin_b,
    count_rows,
    before,
    mine,
    slot_no,
    quad,
    gain,
    mix,
    out_hbm,
    x,
    leg,
    table,
    acc,
    send,
    recv,
    back_send,
    back_recv,
    flat,
    weighted,
    padded,
    pick,
    row_weight,
    table_sum,
    mixed,
    stat_send,
    stat_recv,
    x_sem,
    leg_sem,
    out_sem,
    send_sem,
    recv_sem,
    back_send_sem,
    back_recv_sem,
    stat_sems,
):
    n, slots, longitudes, chunks, points = dims
    me = lax.axis_index("lat")
    quads = n * PAIR * 2
    padded_points = table.shape[2]
    blocks = padded_points // LANES
    degrees = gain.shape[0]

    def peer_of(step):
        far = n - step
        half = (far + 1) // 2
        return lax.rem(me + half * (1 - 2 * lax.rem(far + 1, 2)) + n, n)

    barrier = pltpu.get_barrier_semaphore()

    def greet(step, carry):
        pl.semaphore_signal(
            barrier, inc=1, device_id={"lat": peer_of(step)}, device_id_type=MESH
        )
        return carry

    lax.fori_loop(1, n, greet, 0)

    def x_copy(s):
        return pltpu.make_async_copy(
            x_hbm.at[s], x.at[s, pl.ds(0, longitudes)], x_sem.at[s]
        )

    for s in range(slots):
        x_copy(s).start()
    leg_copy = pltpu.make_async_copy(leg_hbm, leg, leg_sem)
    leg_copy.start()

    band = 32

    def build(i, carry):
        k, r = i // (quads // band), lax.rem(i, quads // band) * band
        r = pl.multiple_of(r, band)
        at = pl.multiple_of(i * band, band)
        c, cb, sb = (ref[pl.ds(at, band), :] for ref in (coef, cos_b, sin_b))
        for a in range(blocks):
            table[k, pl.ds(r, band), a * LANES : (a + 1) * LANES] = (
                c[:, a : a + 1] * cb + c[:, 16 + a : 17 + a] * sb
            ).astype(BF16)
        return carry

    lax.fori_loop(0, chunks * quads // band, build, 0)

    if padded_points > longitudes:
        x[:, longitudes:, :] = jnp.zeros(
            (slots, padded_points - longitudes, x.shape[2]), BF16
        )
    for s in range(slots):
        x_copy(s).wait()

    def fourier(k):
        start = pl.multiple_of(k * quads, quads)
        residual = coef[pl.ds(start, quads), 32:33]

        def one(s, carry):
            values = dot(table[k], x[s])
            values = values - residual * values.astype(BF16).astype(F32)
            flat[pl.ds(0, quads, stride=2), :] = values[:, :LANES]
            flat[pl.ds(1, quads, stride=2), :] = values[:, LANES:]
            send[k, :, s] = (
                flat[pl.ds(0, 2 * quads), :].reshape(n, ROWS, LANES).astype(BF16)
            )
            return carry

        lax.fori_loop(0, slots, one, 0)
        recv[k, me] = send[k, me]

    def exchange(source, target, send_sems, recv_sems, k):
        def one(step, carry):
            peer = peer_of(step)
            pltpu.make_async_remote_copy(
                source.at[k, peer],
                target.at[k, me],
                send_sems.at[k],
                recv_sems.at[k],
                device_id={"lat": peer},
                device_id_type=MESH,
            ).start()
            return carry

        lax.fori_loop(1, n, one, 0)

    def wait_for(buffer, sem):
        part = buffer.at[pl.ds(0, n - 1)]
        pltpu.make_async_copy(part, part, sem).wait()

    fourier(0)

    live = counts[me]
    step_rows = 16 * math.gcd(longitudes // 16, 6)

    def sums(i, carry):
        first, second = carry
        s = i // (longitudes // step_rows)
        r = pl.multiple_of(lax.rem(i, longitudes // step_rows) * step_rows, step_rows)
        on = jnp.where(s < live, 1.0, 0.0).astype(F32)
        values = x[s, pl.ds(r, step_rows), :].astype(F32) * on
        values = values.reshape(step_rows // 8, 8, values.shape[1])
        return first + jnp.sum(values, axis=0), second + jnp.sum(values * values, axis=0)

    zero = jnp.zeros((8, x.shape[2]), F32)
    first, second = lax.fori_loop(
        0, slots * (longitudes // step_rows), sums, (zero, zero)
    )
    first = jnp.sum(first, axis=0, keepdims=True)
    second = jnp.sum(second, axis=0, keepdims=True)
    for i, part in enumerate(
        (first[:, :LANES], first[:, LANES:], second[:, :LANES], second[:, LANES:])
    ):
        stat_send[i : i + 1, :] = part
    stat_recv[me] = stat_send[...]

    pl.semaphore_wait(barrier, n - 1)

    def send_stats(step, carry):
        peer = peer_of(step)
        pltpu.make_async_remote_copy(
            stat_send,
            stat_recv.at[me],
            stat_sems.at[0],
            stat_sems.at[1],
            device_id={"lat": peer},
            device_id_type=MESH,
        ).start()
        return carry

    lax.fori_loop(1, n, send_stats, 0)
    exchange(send, recv, send_sem, recv_sem, 0)
    for k in range(1, chunks):
        fourier(k)
        exchange(send, recv, send_sem, recv_sem, k)

    leg_copy.wait()
    start = dot(before[...], count_rows[...])[:, :1]
    count = dot(mine[...], count_rows[...])[:, :1]
    latitude = lax.broadcasted_iota(jnp.int32, pick.shape, 1).astype(F32)
    hot = (latitude == start + slot_no[...]) & (slot_no[...] < count)
    hot = jnp.where(hot, 1.0, 0.0).astype(F32)
    pick[...] = hot.astype(BF16)
    row_weight[...] = jnp.broadcast_to(
        jnp.sum(hot * quad[...], axis=1, keepdims=True), row_weight.shape
    )

    def pad(w, carry):
        padded[w] = dot(pick[...], leg[w]).astype(BF16)
        return carry

    lax.fori_loop(0, chunks * PAIR, pad, 0)

    inside = lax.broadcasted_iota(jnp.int32, (padded_points, LANES), 0) < longitudes
    ones = jnp.where(inside, 1.0, 0.0).astype(F32).astype(BF16)

    def sum_table(k, carry):
        table_sum[pl.ds(pl.multiple_of(k * quads, quads), quads), :] = dot(table[k], ones)
        return carry

    lax.fori_loop(0, chunks, sum_table, 0)

    wait_for(stat_recv, stat_sems.at[1])
    totals = jnp.sum(stat_recv[...], axis=0)
    mean = totals[0:2] / points
    variance = totals[2:4] / points - mean * mean
    scale = lax.rsqrt(variance + 1e-05)

    rows = n * slots

    def legendre(k, carry):
        wait_for(recv.at[k], recv_sem.at[k])

        def widen(i, inner):
            at = pl.multiple_of(i * slots * ROWS, ROWS)
            flat[pl.ds(at, slots * ROWS), :] = (
                recv[k, i].astype(F32).reshape(slots * ROWS, LANES)
            )
            return inner

        lax.fori_loop(0, n, widen, 0)

        def wave(w, inner):
            number = owner[me * chunks * PAIR + k * PAIR + w]
            is_zero = jnp.where(number == 0, 1.0, 0.0).astype(F32)
            for h in range(2):
                m_h, s_h = mean[h : h + 1], scale[h : h + 1]
                re = flat[pl.ds(w * 4 + h, rows, stride=ROWS), :]
                im = flat[pl.ds(w * 4 + 2 + h, rows, stride=ROWS), :]
                re = re + is_zero * im
                im = im - is_zero * im
                at = k * quads + me * 2 * PAIR + w * 2
                d_re = table_sum[pl.ds(at, 1), :]
                d_im = table_sum[pl.ds(at + 1, 1), :] * (1.0 - is_zero)
                for t, (value, d) in enumerate(((re, d_re), (im, d_im))):
                    left = (2 * t + h) * LANES
                    weighted[:, left : left + LANES] = (
                        ((value - m_h * d) * s_h) * row_weight[...]
                    ).astype(BF16)
            here = padded[k * PAIR + w]
            coefficient = dot(here, weighted[...], (0, 0))
            keep = lax.broadcasted_iota(jnp.int32, (degrees, 1), 0) >= number
            factor = jnp.where(keep, gain[...], 0.0)
            for t in range(2):
                cols = slice(2 * t * LANES, 2 * (t + 1) * LANES)
                filtered = (coefficient[:, cols] * factor).astype(BF16)
                mixed[:, cols] = dot(filtered, mix[...]).astype(BF16)
            synthesis = dot(here, mixed[...])
            for t in range(2):
                doubled = 2.0 - is_zero if t == 0 else 2.0 - 2.0 * is_zero
                for h in range(2):
                    left = (2 * t + h) * LANES
                    flat[pl.ds(w * 4 + t * 2 + h, rows, stride=ROWS), :] = (
                        synthesis[:, left : left + LANES] * doubled
                    )
            return inner

        lax.fori_loop(0, PAIR, wave, 0)

        def narrow(i, inner):
            at = pl.multiple_of(i * slots * ROWS, ROWS)
            back_send[k, i] = (
                flat[pl.ds(at, slots * ROWS), :].reshape(slots, ROWS, LANES).astype(BF16)
            )
            return inner

        lax.fori_loop(0, n, narrow, 0)
        back_recv[k, me] = back_send[k, me]
        exchange(back_send, back_recv, back_send_sem, back_recv_sem, k)
        return carry

    lax.fori_loop(0, chunks, legendre, 0)

    def spread(k, s):
        flat[pl.ds(0, 2 * quads), :] = (
            back_recv[k, :, s].astype(F32).reshape(2 * quads, LANES)
        )
        halves = [flat[pl.ds(h, quads, stride=2), :].astype(BF16) for h in range(2)]
        return dot(table[k], jnp.concatenate(halves, axis=1), (0, 0))

    def out_copy(s):
        return pltpu.make_async_copy(
            x.at[s, pl.ds(0, longitudes)], out_hbm.at[s], out_sem.at[s]
        )

    for k in range(chunks):
        wait_for(back_recv.at[k], back_recv_sem.at[k])

        def one(s, carry, k=k):
            part = spread(k, s)
            if k > 0:
                part = part + acc[s]
            if k < chunks - 1:
                acc[s] = part
            else:
                x[s] = part.astype(BF16)
                out_copy(s).start()
            return carry

        lax.fori_loop(0, slots, one, 0)

    wait_for(stat_recv, stat_sems.at[0])
    for k in range(chunks):
        wait_for(send.at[k], send_sem.at[k])
        wait_for(back_send.at[k], back_send_sem.at[k])
    for s in range(slots):
        out_copy(s).wait()


def angle_tables(waves, longitudes):
    two_pi, factor = 2.0 * math.pi / longitudes, 1.0 / math.sqrt(longitudes)
    part = jnp.arange(waves.shape[0] * 2, dtype=jnp.int32)[:, None] % 2
    waves = jnp.repeat(waves, 2)[:, None]
    lane = jnp.arange(LANES, dtype=jnp.int32)[None, :]
    fine = (waves * lane % longitudes).astype(F32) * two_pi
    coarse = (waves * ((lane % 16) * LANES % longitudes) % longitudes).astype(F32) * two_pi
    cos_a, sin_a = jnp.cos(coarse) * factor, jnp.sin(coarse) * factor
    first = jnp.where((part == 0) | (waves == 0), cos_a, -sin_a)
    second = jnp.where(part == 0, -sin_a, -cos_a)
    residual = jnp.where((part == 1) & (waves == 0), 1.0, 0.0).astype(F32)
    coef = jnp.where(lane < 16, first, jnp.where(lane < 32, second, residual))
    return coef, jnp.cos(fine), jnp.sin(fine)


def body(
    grid_values, lat_counts, owner_wavenumber, legendre, quad_weight, spectral_gain, channel_mix
):
    slots, longitudes, channels = grid_values.shape
    n = lat_counts.shape[0]
    share, live_total, degrees = legendre.shape
    chunks = share // PAIR
    blocks = -(-longitudes // LANES)
    padded_points = blocks * LANES
    quads = n * PAIR * 2
    rows = n * slots
    ordered = owner_wavenumber.reshape(n, chunks, PAIR).transpose(1, 0, 2).reshape(-1)
    coef, cos_b, sin_b = angle_tables(ordered, longitudes)
    holder = np.arange(rows)[:, None] // slots
    device = np.arange(n)[None, :]
    before = jnp.asarray(device < holder, BF16)
    mine = jnp.asarray(device == holder, BF16)
    slot_no = jnp.asarray(np.arange(rows)[:, None] % slots, F32)
    count_rows = jnp.broadcast_to(lat_counts.astype(BF16)[:, None], (n, LANES))
    smem = pl.BlockSpec(memory_space=pltpu.SMEM)
    vmem = pl.BlockSpec(memory_space=pltpu.VMEM)
    anywhere = pl.BlockSpec(memory_space=pl.ANY)
    message = (chunks, n, slots, ROWS, LANES)
    dma = pltpu.SemaphoreType.DMA
    dims = (n, slots, longitudes, chunks, live_total * longitudes)
    return pl.pallas_call(
        functools.partial(kernel, dims),
        out_shape=jax.ShapeDtypeStruct(grid_values.shape, BF16),
        in_specs=[smem, smem, anywhere, anywhere] + [vmem] * 10,
        out_specs=anywhere,
        scratch_shapes=[
            pltpu.VMEM((slots, padded_points, channels), BF16),
            pltpu.VMEM((share, live_total, degrees), BF16),
            pltpu.VMEM((chunks, quads, padded_points), BF16),
            pltpu.VMEM((slots, padded_points, channels), F32),
            pltpu.VMEM(message, BF16),
            pltpu.VMEM(message, BF16),
            pltpu.VMEM(message, BF16),
            pltpu.VMEM(message, BF16),
            pltpu.VMEM((max(rows * ROWS, 2 * quads), LANES), F32),
            pltpu.VMEM((rows, 2 * channels), BF16),
            pltpu.VMEM((share, rows, degrees), BF16),
            pltpu.VMEM((rows, live_total), BF16),
            pltpu.VMEM((rows, LANES), F32),
            pltpu.VMEM((chunks * quads, LANES), F32),
            pltpu.VMEM((degrees, 2 * channels), BF16),
            pltpu.VMEM((4, LANES), F32),
            pltpu.VMEM((n, 4, LANES), F32),
            dma((slots,)),
            dma,
            dma((slots,)),
            dma((chunks,)),
            dma((chunks,)),
            dma((chunks,)),
            dma((chunks,)),
            dma((2,)),
        ],
        compiler_params=pltpu.CompilerParams(
            collective_id=0, has_side_effects=True, vmem_limit_bytes=60 * 1024 * 1024
        ),
    )(
        lat_counts,
        owner_wavenumber,
        grid_values,
        legendre,
        coef,
        cos_b,
        sin_b,
        count_rows,
        before,
        mine,
        slot_no,
        quad_weight[None, :],
        spectral_gain,
        channel_mix,
    )


def solution(mesh):
    return jax.shard_map(
        body,
        mesh=mesh,
        in_specs=(P(("group", "lat"), None, None), P(), P(), P("lat", None, None), P(), P(), P()),
        out_specs=P(("group", "lat"), None, None),
        check_vma=False,
    )
```

```python
import functools
import math

import jax
import jax.numpy as jnp
import numpy as np
from jax import lax
from jax.experimental import pallas as pl
from jax.experimental.pallas import tpu as pltpu
from jax.sharding import PartitionSpec as P

MESH = pl.DeviceIdType.MESH
LANES = 128
PAIR = 2
ROWS = 8
BF16, F32 = jnp.bfloat16, jnp.float32


def dot(a, b, contract=(1, 0)):
    return lax.dot_general(
        a, b, (((contract[0],), (contract[1],)), ((), ())), preferred_element_type=F32
    )


def kernel(
    dims,
    counts,
    owner,
    x_hbm,
    waves_hbm,
    leg_hbm,
    number_hbm,
    count_hbm,
    quad_hbm,
    gain_hbm,
    mix_hbm,
    out,
    x,
    waves,
    leg,
    number_row,
    count_row,
    quad,
    gain,
    mix,
    table,
    turned,
    acc,
    send,
    recv,
    back_send,
    back_recv,
    flat,
    weighted,
    padded,
    row_weight,
    table_sum,
    mixed,
    stat_mine,
    stat_pair,
    stat_send,
    stat_recv,
    stat_total,
    x_sem,
    load_sem,
    send_sem,
    recv_sem,
    back_send_sem,
    back_recv_sem,
    pair_sems,
    stat_sems,
    total_sems,
):
    n, slots, longitudes, chunks, points = dims
    me = lax.axis_index("lat")
    quads = n * PAIR * 2
    half_points = longitudes // 2
    padded_half = table.shape[2] // 2
    padded_points = 2 * padded_half
    degrees = gain.shape[0]
    chips, chip, core = n // 2, me // 2, lax.rem(me, 2)
    partner = me + 1 - 2 * core
    last = chunks - 1
    early = slots - 1

    def ring(here, size, step):
        far = size - step
        half = (far + 1) // 2
        return lax.rem(here + half * (1 - 2 * lax.rem(far + 1, 2)) + size, size)

    def peer_of(step):
        return ring(me, n, step)

    barrier = pltpu.get_barrier_semaphore()

    def greet(step, carry):
        pl.semaphore_signal(
            barrier, inc=1, device_id={"lat": peer_of(step)}, device_id_type=MESH
        )
        return carry

    lax.fori_loop(1, n, greet, 0)

    loads = [
        pltpu.make_async_copy(source, target, load_sem.at[i])
        for i, (source, target) in enumerate(
            (
                (number_hbm, number_row),
                (waves_hbm, waves),
                (leg_hbm, leg),
                (count_hbm, count_row),
                (quad_hbm, quad),
                (gain_hbm, gain),
                (mix_hbm, mix),
            )
        )
    ]

    def x_copy(s, h):
        return pltpu.make_async_copy(
            x_hbm.at[s, pl.ds(h * half_points, half_points)],
            x.at[s, pl.ds(h * padded_half, half_points)],
            x_sem.at[s, h],
        )

    halves = [(s, h) for s in range(slots) for h in range(2)]
    for load in loads[:2]:
        load.start()
    for s, h in halves:
        x_copy(s, h).start()
    for load in loads[2:]:
        load.start()

    if padded_half > half_points:
        for h in range(2):
            x[:, h * padded_half + half_points : (h + 1) * padded_half, :] = jnp.zeros(
                (slots, padded_half - half_points, x.shape[2]), BF16
            )
    for load in loads[:2]:
        load.wait()

    def build(k):
        q, r = (lax.broadcasted_iota(jnp.int32, (quads, LANES), i) for i in range(2))
        slot = (q // (2 * PAIR)) * (chunks * PAIR) + k * PAIR + lax.rem(q // 2, PAIR)
        held = jnp.zeros((quads, LANES), F32)
        for i in range(number_row.shape[0]):
            numbers = number_row[i : i + 1, :].astype(F32)
            held = held + jnp.where(slot == r + i * LANES, numbers, 0.0)
        part = lax.rem(lax.broadcasted_iota(jnp.int32, (quads, 1), 0), 2).astype(F32)
        code = 2.0 * jnp.sum(held, axis=1, keepdims=True) + part
        column = lax.broadcasted_iota(jnp.int32, (quads, waves.shape[0]), 1).astype(F32)
        hot = jnp.where(column == code, 1.0, 0.0).astype(F32).astype(BF16)
        rows = dot(hot, waves[...])
        first, sign = rows[:, :padded_half], rows[:, padded_half : padded_half + 1]
        table[k, :, :padded_half] = first.astype(BF16)
        table[k, :, padded_half:] = (first * sign).astype(BF16)
        return rows[:, padded_half + 1 : padded_half + 2]

    def fourier(k):
        residual = build(k)

        def one(s, carry):
            if k == 0:
                for h in range(2):
                    x_copy(s, h).wait()
            values = dot(table[k], x[s])
            values = values - residual * values.astype(BF16).astype(F32)
            flat[pl.ds(0, quads, stride=2), :] = values[:, :LANES]
            flat[pl.ds(1, quads, stride=2), :] = values[:, LANES:]
            send[k, :, s] = (
                flat[pl.ds(0, 2 * quads), :].reshape(n, ROWS, LANES).astype(BF16)
            )
            return carry

        lax.fori_loop(0, slots, one, 0)
        recv[k, me] = send[k, me]

    def exchange(source, target, send_sems, recv_sems, k, part=None, at=None):
        def cut(ref, i):
            return ref.at[k, i] if part is None else ref.at[k, i, pl.ds(*part)]

        at = k if at is None else at

        def one(step, carry):
            peer = peer_of(step)
            pltpu.make_async_remote_copy(
                cut(source, peer),
                cut(target, me),
                send_sems.at[at],
                recv_sems.at[at],
                device_id={"lat": peer},
                device_id_type=MESH,
            ).start()
            return carry

        lax.fori_loop(1, n, one, 0)

    def wait_for(buffer, sem):
        pltpu.make_async_copy(buffer, buffer, sem).wait()

    def others(buffer, k):
        return buffer.at[k, pl.ds(0, n - 1)]

    fourier(0)
    pl.semaphore_wait(barrier, n - 1)
    exchange(send, recv, send_sem, recv_sem, 0)

    live = counts[me]
    step_rows = 96

    def sums(i, carry):
        first, second = carry
        s = i // (padded_points // step_rows)
        r = pl.multiple_of(lax.rem(i, padded_points // step_rows) * step_rows, step_rows)
        on = jnp.where(s < live, 1.0, 0.0).astype(F32)
        values = x[s, pl.ds(r, step_rows), :].astype(F32) * on
        values = values.reshape(step_rows // 8, 8, values.shape[1])
        return first + jnp.sum(values, axis=0), second + jnp.sum(values * values, axis=0)

    zero = jnp.zeros((8, x.shape[2]), F32)
    first, second = lax.fori_loop(
        0, slots * (padded_points // step_rows), sums, (zero, zero)
    )
    first = jnp.sum(first, axis=0, keepdims=True)
    second = jnp.sum(second, axis=0, keepdims=True)
    for i, part in enumerate((first, second)):
        for h in range(2):
            stat_mine[i, h : h + 1, :] = part[:, h * LANES : (h + 1) * LANES]

    def pair_copy(source, target, sems):
        return pltpu.make_async_remote_copy(
            source, target, sems.at[0], sems.at[1], device_id={"lat": partner}, device_id_type=MESH
        )

    to_partner = pair_copy(stat_mine.at[1 - core], stat_pair, pair_sems)
    to_partner.start()
    for k in range(1, chunks):
        fourier(k)
        if k == 1:
            to_partner.wait()
            stat_send[...] = stat_mine[core] + stat_pair[...]
            stat_recv[chip] = stat_send[...]

            def send_stats(step, carry):
                pltpu.make_async_remote_copy(
                    stat_send,
                    stat_recv.at[chip],
                    stat_sems.at[0],
                    stat_sems.at[1],
                    device_id={"lat": ring(chip, chips, step) * 2 + core},
                    device_id_type=MESH,
                ).start()
                return carry

            lax.fori_loop(1, chips, send_stats, 0)
        exchange(send, recv, send_sem, recv_sem, k)

    for load in loads[2:]:
        load.wait()
    row = lax.broadcasted_iota(jnp.int32, (n * slots, n), 0)
    device = lax.broadcasted_iota(jnp.int32, (n * slots, n), 1)
    holder, slot_no = row // slots, lax.rem(row[:, :1], slots).astype(F32)
    number_live = count_row[...].astype(F32)
    start = jnp.sum(jnp.where(device < holder, number_live, 0.0), axis=1, keepdims=True)
    count = jnp.sum(jnp.where(device == holder, number_live, 0.0), axis=1, keepdims=True)
    latitude = lax.broadcasted_iota(jnp.int32, (n * slots, leg.shape[1]), 1).astype(F32)
    hot = (latitude == start + slot_no) & (slot_no < count)
    hot = jnp.where(hot, 1.0, 0.0).astype(F32)
    held = jnp.zeros(row_weight.shape, F32)
    for i in range(quad.shape[0]):
        held = held + hot[:, i * LANES : (i + 1) * LANES] * quad[i : i + 1, :]
    row_weight[...] = jnp.broadcast_to(
        jnp.sum(held, axis=1, keepdims=True), row_weight.shape
    )
    pick = hot.astype(BF16)

    def pad(w, carry):
        padded[w] = dot(pick, leg[w]).astype(BF16)
        return carry

    lax.fori_loop(0, chunks * PAIR, pad, 0)

    point = lax.rem(lax.broadcasted_iota(jnp.int32, (padded_points, LANES), 0), padded_half)
    ones = jnp.where(point < half_points, 1.0, 0.0).astype(F32).astype(BF16)

    def sum_table(k, carry):
        table_sum[pl.ds(pl.multiple_of(k * quads, quads), quads), :] = dot(table[k], ones)
        return carry

    lax.fori_loop(0, chunks, sum_table, 0)
    r, c = (lax.broadcasted_iota(jnp.int32, (quads, quads), i) for i in range(2))
    unit = jnp.where(r == c, 1.0, 0.0).astype(F32).astype(BF16)
    turned[...] = dot(table[last], unit, (0, 0)).astype(BF16)

    wait_for(stat_recv.at[pl.ds(0, chips - 1)], stat_sems.at[1])
    stat_total[core] = jnp.sum(stat_recv[...], axis=0)
    total_copy = pair_copy(stat_total.at[core], stat_total.at[core], total_sems)
    total_copy.start()
    total_copy.wait()
    mean = stat_total[0] / points
    variance = stat_total[1] / points - mean * mean
    scale = lax.rsqrt(variance + 1e-05)

    rows = n * slots

    def legendre(k, carry):
        wait_for(others(recv, k), recv_sem.at[k])

        def widen(i, inner):
            at = pl.multiple_of(i * slots * ROWS, ROWS)
            flat[pl.ds(at, slots * ROWS), :] = (
                recv[k, i].astype(F32).reshape(slots * ROWS, LANES)
            )
            return inner

        lax.fori_loop(0, n, widen, 0)

        def wave(w, inner):
            number = owner[me * chunks * PAIR + k * PAIR + w]
            is_zero = jnp.where(number == 0, 1.0, 0.0).astype(F32)
            for h in range(2):
                m_h, s_h = mean[h : h + 1], scale[h : h + 1]
                re = flat[pl.ds(w * 4 + h, rows, stride=ROWS), :]
                im = flat[pl.ds(w * 4 + 2 + h, rows, stride=ROWS), :]
                re = re + is_zero * im
                im = im - is_zero * im
                at = k * quads + me * 2 * PAIR + w * 2
                d_re = table_sum[pl.ds(at, 1), :]
                d_im = table_sum[pl.ds(at + 1, 1), :] * (1.0 - is_zero)
                for t, (value, d) in enumerate(((re, d_re), (im, d_im))):
                    left = (2 * t + h) * LANES
                    weighted[:, left : left + LANES] = (
                        ((value - m_h * d) * s_h) * row_weight[...]
                    ).astype(BF16)
            here = padded[k * PAIR + w]
            coefficient = dot(here, weighted[...], (0, 0))
            keep = lax.broadcasted_iota(jnp.int32, (degrees, 1), 0) >= number
            factor = jnp.where(keep, gain[...], 0.0)
            for t in range(2):
                cols = slice(2 * t * LANES, 2 * (t + 1) * LANES)
                filtered = (coefficient[:, cols] * factor).astype(BF16)
                mixed[:, cols] = dot(filtered, mix[...]).astype(BF16)
            synthesis = dot(here, mixed[...])
            for t in range(2):
                doubled = 2.0 - is_zero if t == 0 else 2.0 - 2.0 * is_zero
                for h in range(2):
                    left = (2 * t + h) * LANES
                    flat[pl.ds(w * 4 + t * 2 + h, rows, stride=ROWS), :] = (
                        synthesis[:, left : left + LANES] * doubled
                    )
            return inner

        lax.fori_loop(0, PAIR, wave, 0)

        def narrow(i, inner):
            at = pl.multiple_of(i * slots * ROWS, ROWS)
            back_send[k, i] = (
                flat[pl.ds(at, slots * ROWS), :].reshape(slots, ROWS, LANES).astype(BF16)
            )
            return inner

        lax.fori_loop(0, n, narrow, 0)
        back_recv[k, me] = back_send[k, me]
        return carry

    def legendre_and_return(k, carry):
        legendre(k, carry)
        exchange(back_send, back_recv, back_send_sem, back_recv_sem, k)
        return carry

    lax.fori_loop(0, last, legendre_and_return, 0)
    legendre(last, 0)
    parts = ((0, early), (early, slots - early))
    for i, part in enumerate(parts):
        exchange(back_send, back_recv, back_send_sem, back_recv_sem, last, part, last + i)

    def spread(k, s):
        flat[pl.ds(0, 2 * quads), :] = (
            back_recv[k, :, s].astype(F32).reshape(2 * quads, LANES)
        )
        both = [flat[pl.ds(h, quads, stride=2), :].astype(BF16) for h in range(2)]
        return jnp.concatenate(both, axis=1)

    for k in range(last):
        wait_for(others(back_recv, k), back_recv_sem.at[k])

        def add(s, carry, k=k):
            part = dot(table[k], spread(k, s), (0, 0))
            acc[s] = part if k == 0 else part + acc[s]
            return carry

        lax.fori_loop(0, slots, add, 0)

    def finish(s, carry):
        total = dot(turned[...], spread(last, s)) + acc[s]
        for h in range(2):
            out[s, h * half_points : (h + 1) * half_points, :] = total[
                h * padded_half : h * padded_half + half_points
            ].astype(BF16)
        return carry

    def piece(buffer, part):
        return buffer.at[last, pl.ds(0, n - 1), pl.ds(*part)]

    for k in range(chunks):
        wait_for(others(send, k), send_sem.at[k])
    for k in range(last):
        wait_for(others(back_send, k), back_send_sem.at[k])
    wait_for(stat_recv.at[pl.ds(0, chips - 1)], stat_sems.at[0])
    for i, (first_slot, size) in enumerate(parts):
        wait_for(piece(back_recv, parts[i]), back_recv_sem.at[last + i])
        lax.fori_loop(first_slot, first_slot + size, finish, 0)
    for i, part in enumerate(parts):
        wait_for(piece(back_send, part), back_send_sem.at[last + i])


def wave_rows(wave_count, longitudes, padded_half):
    half = longitudes // 2
    number = np.arange(wave_count)
    phase = number[:, None] * np.arange(half)[None, :] % longitudes
    angle = phase * (2.0 * math.pi / longitudes)
    sine = np.where(number[:, None] > 0, -np.sin(angle), np.cos(angle))
    rows = np.zeros((wave_count, 2, padded_half + LANES), np.float32)
    rows[:, :, :half] = np.stack([np.cos(angle), sine], axis=1) / math.sqrt(longitudes)
    rows[:, :, padded_half] = 1.0 - 2.0 * (number % 2)[:, None]
    rows[0, 1, padded_half + 1] = 1.0
    return jnp.asarray(rows.reshape(2 * wave_count, -1), BF16)


def body(
    grid_values, lat_counts, owner_wavenumber, legendre, quad_weight, spectral_gain, channel_mix
):
    slots, longitudes, channels = grid_values.shape
    n = lat_counts.shape[0]
    share, live_total, degrees = legendre.shape
    chunks = share // PAIR
    padded_half = -(-longitudes // (2 * 256)) * 256
    padded_points = 2 * padded_half
    quads = n * PAIR * 2
    rows = n * slots
    waves = wave_rows(owner_wavenumber.shape[0], longitudes, padded_half)
    smem = pl.BlockSpec(memory_space=pltpu.SMEM)
    anywhere = pl.BlockSpec(memory_space=pl.ANY)
    message = (chunks, n, slots, ROWS, LANES)
    dma = pltpu.SemaphoreType.DMA
    dims = (n, slots, longitudes, chunks, live_total * longitudes)
    return pl.pallas_call(
        functools.partial(kernel, dims),
        out_shape=pltpu.VMEM(grid_values.shape, BF16),
        in_specs=[smem, smem] + [anywhere] * 8,
        out_specs=pl.BlockSpec(memory_space=pltpu.VMEM),
        scratch_shapes=[
            pltpu.VMEM((slots, padded_points, channels), BF16),
            pltpu.VMEM(waves.shape, BF16),
            pltpu.VMEM((share, live_total, degrees), BF16),
            pltpu.VMEM((owner_wavenumber.shape[0] // LANES, LANES), jnp.int32),
            pltpu.VMEM((1, n), jnp.int32),
            pltpu.VMEM((live_total // LANES, LANES), F32),
            pltpu.VMEM((degrees, channels), F32),
            pltpu.VMEM((channels, channels), BF16),
            pltpu.VMEM((chunks, quads, padded_points), BF16),
            pltpu.VMEM((padded_points, quads), BF16),
            pltpu.VMEM((slots, padded_points, channels), F32),
            pltpu.VMEM(message, BF16),
            pltpu.VMEM(message, BF16),
            pltpu.VMEM(message, BF16),
            pltpu.VMEM(message, BF16),
            pltpu.VMEM((max(rows * ROWS, 2 * quads), LANES), F32),
            pltpu.VMEM((rows, 2 * channels), BF16),
            pltpu.VMEM((share, rows, degrees), BF16),
            pltpu.VMEM((rows, LANES), F32),
            pltpu.VMEM((chunks * quads, LANES), F32),
            pltpu.VMEM((degrees, 2 * channels), BF16),
            pltpu.VMEM((2, 2, LANES), F32),
            pltpu.VMEM((2, LANES), F32),
            pltpu.VMEM((2, LANES), F32),
            pltpu.VMEM((n // 2, 2, LANES), F32),
            pltpu.VMEM((2, 2, LANES), F32),
            dma((slots, 2)),
            dma((7,)),
            dma((chunks,)),
            dma((chunks,)),
            dma((chunks + 1,)),
            dma((chunks + 1,)),
            dma((2,)),
            dma((2,)),
            dma((2,)),
        ],
        compiler_params=pltpu.CompilerParams(
            collective_id=0, has_side_effects=True, vmem_limit_bytes=54 * 1024 * 1024
        ),
    )(
        lat_counts,
        owner_wavenumber,
        grid_values,
        waves,
        legendre,
        owner_wavenumber.reshape(-1, LANES),
        lat_counts[None, :],
        quad_weight.reshape(-1, LANES),
        spectral_gain,
        channel_mix,
    )


def solution(mesh):
    return jax.shard_map(
        body,
        mesh=mesh,
        in_specs=(P(("group", "lat"), None, None), P(), P(), P("lat", None, None), P(), P(), P()),
        out_specs=P(("group", "lat"), None, None),
        check_vma=False,
    )
```

```python
import functools
import math

import jax
import jax.numpy as jnp
import numpy as np
from jax import lax
from jax.experimental import pallas as pl
from jax.experimental.pallas import tpu as pltpu
from jax.sharding import PartitionSpec as P

MESH = pl.DeviceIdType.MESH
LANES = 128
PAIR = 2
ROWS = 8
BF16, F32 = jnp.bfloat16, jnp.float32


def dot(a, b, contract=(1, 0)):
    return lax.dot_general(
        a, b, (((contract[0],), (contract[1],)), ((), ())), preferred_element_type=F32
    )


def kernel(
    dims,
    counts,
    owner,
    x_hbm,
    waves_hbm,
    leg_hbm,
    number_hbm,
    count_hbm,
    quad_hbm,
    gain_hbm,
    mix_hbm,
    out,
    x,
    waves,
    leg,
    number_row,
    count_row,
    quad,
    gain,
    mix,
    table,
    turned,
    acc,
    send,
    recv,
    back_send,
    back_recv,
    flat,
    weighted,
    padded,
    row_weight,
    table_sum,
    mixed,
    stat_mine,
    stat_pair,
    stat_send,
    stat_recv,
    block_send,
    block_recv,
    stat_total,
    x_sem,
    load_sem,
    send_sem,
    recv_sem,
    back_send_sem,
    back_recv_sem,
    pair_sems,
    stat_sems,
    block_sems,
    total_sems,
    far_sem,
):
    n, slots, longitudes, chunks, points = dims
    me = lax.axis_index("lat")
    quads = n * PAIR * 2
    half_points = longitudes // 2
    padded_half = table.shape[2] // 2
    padded_points = 2 * padded_half
    degrees = gain.shape[0]
    chips, chip, core = n // 2, me // 2, lax.rem(me, 2)
    partner = me + 1 - 2 * core
    last = chunks - 1
    early = slots - 1

    def ring(here, size, step):
        far = size - step
        half = (far + 1) // 2
        return lax.rem(here + half * (1 - 2 * lax.rem(far + 1, 2)) + size, size)

    def peer_of(step):
        return ring(me, n, step)

    barrier = pltpu.get_barrier_semaphore()
    near_from = n - n // 2

    def greet(step, carry):
        pl.semaphore_signal(
            barrier, inc=1, device_id={"lat": peer_of(step)}, device_id_type=MESH
        )
        return carry

    lax.fori_loop(near_from, n, greet, 0)

    loads = [
        pltpu.make_async_copy(source, target, load_sem.at[i])
        for i, (source, target) in enumerate(
            (
                (number_hbm, number_row),
                (waves_hbm, waves),
                (leg_hbm, leg),
                (count_hbm, count_row),
                (quad_hbm, quad),
                (gain_hbm, gain),
                (mix_hbm, mix),
            )
        )
    ]

    def x_copy(s, h):
        return pltpu.make_async_copy(
            x_hbm.at[s, pl.ds(h * half_points, half_points)],
            x.at[s, pl.ds(h * padded_half, half_points)],
            x_sem.at[s, h],
        )

    halves = [(s, h) for s in range(slots) for h in range(2)]
    for load in loads[:2]:
        load.start()
    for s, h in halves:
        x_copy(s, h).start()
    for load in loads[2:]:
        load.start()

    if padded_half > half_points:
        for h in range(2):
            x[:, h * padded_half + half_points : (h + 1) * padded_half, :] = jnp.zeros(
                (slots, padded_half - half_points, x.shape[2]), BF16
            )
    for load in loads[:2]:
        load.wait()

    def build(k):
        q, r = (lax.broadcasted_iota(jnp.int32, (quads, LANES), i) for i in range(2))
        slot = (q // (2 * PAIR)) * (chunks * PAIR) + k * PAIR + lax.rem(q // 2, PAIR)
        held = jnp.zeros((quads, LANES), F32)
        for i in range(number_row.shape[0]):
            numbers = number_row[i : i + 1, :].astype(F32)
            held = held + jnp.where(slot == r + i * LANES, numbers, 0.0)
        part = lax.rem(lax.broadcasted_iota(jnp.int32, (quads, 1), 0), 2).astype(F32)
        code = 2.0 * jnp.sum(held, axis=1, keepdims=True) + part
        column = lax.broadcasted_iota(jnp.int32, (quads, waves.shape[0]), 1).astype(F32)
        hot = jnp.where(column == code, 1.0, 0.0).astype(F32).astype(BF16)
        rows = dot(hot, waves[...])
        first, sign = rows[:, :padded_half], rows[:, padded_half : padded_half + 1]
        table[k, :, :padded_half] = first.astype(BF16)
        table[k, :, padded_half:] = (first * sign).astype(BF16)
        return rows[:, padded_half + 1 : padded_half + 2]

    def fourier(k):
        residual = build(k)

        def one(s, carry):
            if k == 0:
                for h in range(2):
                    x_copy(s, h).wait()
            values = dot(table[k], x[s])
            values = values - residual * values.astype(BF16).astype(F32)
            flat[pl.ds(0, quads, stride=2), :] = values[:, :LANES]
            flat[pl.ds(1, quads, stride=2), :] = values[:, LANES:]
            send[k, :, s] = (
                flat[pl.ds(0, 2 * quads), :].reshape(n, ROWS, LANES).astype(BF16)
            )
            return carry

        cut = slots - 2 if k == 0 else slots
        lax.fori_loop(0, cut, one, 0)
        if k == 0:
            pl.semaphore_wait(barrier, n // 2)
            for edge in (n // 4, n - n // 4):
                pl.semaphore_signal(
                    far_sem, inc=1, device_id={"lat": lax.rem(me + edge, n)}, device_id_type=MESH
                )
        lax.fori_loop(cut, slots, one, 0)
        recv[k, me] = send[k, me]

    def exchange(source, target, send_sems, recv_sems, k, part=None, at=None, steps=(1, n)):
        def cut(ref, i):
            return ref.at[k, i] if part is None else ref.at[k, i, pl.ds(*part)]

        at = k if at is None else at

        def one(step, carry):
            peer = peer_of(step)
            pltpu.make_async_remote_copy(
                cut(source, peer),
                cut(target, me),
                send_sems.at[at],
                recv_sems.at[at],
                device_id={"lat": peer},
                device_id_type=MESH,
            ).start()
            return carry

        lax.fori_loop(*steps, one, 0)

    def wait_for(buffer, sem):
        pltpu.make_async_copy(buffer, buffer, sem).wait()

    def others(buffer, k):
        return buffer.at[k, pl.ds(0, n - 1)]

    fourier(0)
    exchange(send, recv, send_sem, recv_sem, 0, steps=(near_from, n))
    pl.semaphore_wait(far_sem, 2)
    exchange(send, recv, send_sem, recv_sem, 0, steps=(1, near_from))

    live = counts[me]
    step_rows = 96

    def sums(i, carry):
        first, second = carry
        s = i // (padded_points // step_rows)
        r = pl.multiple_of(lax.rem(i, padded_points // step_rows) * step_rows, step_rows)
        on = jnp.where(s < live, 1.0, 0.0).astype(F32)
        values = x[s, pl.ds(r, step_rows), :].astype(F32) * on
        values = values.reshape(step_rows // 8, 8, values.shape[1])
        return first + jnp.sum(values, axis=0), second + jnp.sum(values * values, axis=0)

    zero = jnp.zeros((8, x.shape[2]), F32)
    first, second = lax.fori_loop(
        0, slots * (padded_points // step_rows), sums, (zero, zero)
    )
    first = jnp.sum(first, axis=0, keepdims=True)
    second = jnp.sum(second, axis=0, keepdims=True)
    for i, part in enumerate((first, second)):
        for h in range(2):
            stat_mine[i, h : h + 1, :] = part[:, h * LANES : (h + 1) * LANES]

    def pair_copy(source, target, sems):
        return pltpu.make_async_remote_copy(
            source, target, sems.at[0], sems.at[1], device_id={"lat": partner}, device_id_type=MESH
        )

    block = stat_recv.shape[0]
    rank, lane = chip // block, lax.rem(chip, block)

    def stat_copies(source, target, here, size, chip_of, sems):
        def one(step, carry):
            pltpu.make_async_remote_copy(
                source,
                target.at[here],
                sems.at[0],
                sems.at[1],
                device_id={"lat": chip_of(ring(here, size, step)) * 2 + core},
                device_id_type=MESH,
            ).start()
            return carry

        lax.fori_loop(1, size, one, 0)

    to_partner = pair_copy(stat_mine.at[1 - core], stat_pair, pair_sems)
    to_partner.start()
    for k in range(1, chunks):
        fourier(k)
        if k == 1:
            to_partner.wait()
            stat_send[...] = stat_mine[core] + stat_pair[...]
            stat_recv[lane] = stat_send[...]
            stat_copies(stat_send, stat_recv, lane, block, lambda i: rank * block + i, stat_sems)
        if k == last:
            wait_for(stat_recv.at[pl.ds(0, block - 1)], stat_sems.at[1])
            block_send[...] = jnp.sum(stat_recv[...], axis=0)
            block_recv[rank] = block_send[...]
            stat_copies(
                block_send, block_recv, rank, chips // block, lambda i: i * block + lane, block_sems
            )
        exchange(send, recv, send_sem, recv_sem, k)

    for load in loads[2:]:
        load.wait()
    row = lax.broadcasted_iota(jnp.int32, (n * slots, n), 0)
    device = lax.broadcasted_iota(jnp.int32, (n * slots, n), 1)
    holder, slot_no = row // slots, lax.rem(row[:, :1], slots).astype(F32)
    number_live = count_row[...].astype(F32)
    start = jnp.sum(jnp.where(device < holder, number_live, 0.0), axis=1, keepdims=True)
    count = jnp.sum(jnp.where(device == holder, number_live, 0.0), axis=1, keepdims=True)
    latitude = lax.broadcasted_iota(jnp.int32, (n * slots, leg.shape[1]), 1).astype(F32)
    hot = (latitude == start + slot_no) & (slot_no < count)
    hot = jnp.where(hot, 1.0, 0.0).astype(F32)
    held = jnp.zeros(row_weight.shape, F32)
    for i in range(quad.shape[0]):
        held = held + hot[:, i * LANES : (i + 1) * LANES] * quad[i : i + 1, :]
    row_weight[...] = jnp.broadcast_to(
        jnp.sum(held, axis=1, keepdims=True), row_weight.shape
    )
    pick = hot.astype(BF16)

    def pad(w, carry):
        padded[w] = dot(pick, leg[w]).astype(BF16)
        return carry

    lax.fori_loop(0, chunks * PAIR, pad, 0)

    point = lax.rem(lax.broadcasted_iota(jnp.int32, (padded_points, LANES), 0), padded_half)
    ones = jnp.where(point < half_points, 1.0, 0.0).astype(F32).astype(BF16)

    def sum_table(k, carry):
        table_sum[pl.ds(pl.multiple_of(k * quads, quads), quads), :] = dot(table[k], ones)
        return carry

    lax.fori_loop(0, chunks, sum_table, 0)
    r, c = (lax.broadcasted_iota(jnp.int32, (quads, quads), i) for i in range(2))
    unit = jnp.where(r == c, 1.0, 0.0).astype(F32).astype(BF16)
    turned[...] = dot(table[last], unit, (0, 0)).astype(BF16)

    wait_for(block_recv.at[pl.ds(0, chips // block - 1)], block_sems.at[1])
    stat_total[core] = jnp.sum(block_recv[...], axis=0)
    total_copy = pair_copy(stat_total.at[core], stat_total.at[core], total_sems)
    total_copy.start()
    total_copy.wait()
    mean = stat_total[0] / points
    variance = stat_total[1] / points - mean * mean
    scale = lax.rsqrt(variance + 1e-05)

    rows = n * slots

    def legendre(k, carry):
        wait_for(others(recv, k), recv_sem.at[k])

        def widen(i, inner):
            at = pl.multiple_of(i * slots * ROWS, ROWS)
            flat[pl.ds(at, slots * ROWS), :] = (
                recv[k, i].astype(F32).reshape(slots * ROWS, LANES)
            )
            return inner

        lax.fori_loop(0, n, widen, 0)

        def wave(w, inner):
            number = owner[me * chunks * PAIR + k * PAIR + w]
            is_zero = jnp.where(number == 0, 1.0, 0.0).astype(F32)
            for h in range(2):
                m_h, s_h = mean[h : h + 1], scale[h : h + 1]
                re = flat[pl.ds(w * 4 + h, rows, stride=ROWS), :]
                im = flat[pl.ds(w * 4 + 2 + h, rows, stride=ROWS), :]
                re = re + is_zero * im
                im = im - is_zero * im
                at = k * quads + me * 2 * PAIR + w * 2
                d_re = table_sum[pl.ds(at, 1), :]
                d_im = table_sum[pl.ds(at + 1, 1), :] * (1.0 - is_zero)
                for t, (value, d) in enumerate(((re, d_re), (im, d_im))):
                    left = (2 * t + h) * LANES
                    weighted[:, left : left + LANES] = (
                        ((value - m_h * d) * s_h) * row_weight[...]
                    ).astype(BF16)
            here = padded[k * PAIR + w]
            coefficient = dot(here, weighted[...], (0, 0))
            keep = lax.broadcasted_iota(jnp.int32, (degrees, 1), 0) >= number
            factor = jnp.where(keep, gain[...], 0.0)
            for t in range(2):
                cols = slice(2 * t * LANES, 2 * (t + 1) * LANES)
                filtered = (coefficient[:, cols] * factor).astype(BF16)
                mixed[:, cols] = dot(filtered, mix[...]).astype(BF16)
            synthesis = dot(here, mixed[...])
            for t in range(2):
                doubled = 2.0 - is_zero if t == 0 else 2.0 - 2.0 * is_zero
                for h in range(2):
                    left = (2 * t + h) * LANES
                    flat[pl.ds(w * 4 + t * 2 + h, rows, stride=ROWS), :] = (
                        synthesis[:, left : left + LANES] * doubled
                    )
            return inner

        lax.fori_loop(0, PAIR, wave, 0)

        def narrow(i, inner):
            at = pl.multiple_of(i * slots * ROWS, ROWS)
            back_send[k, i] = (
                flat[pl.ds(at, slots * ROWS), :].reshape(slots, ROWS, LANES).astype(BF16)
            )
            return inner

        lax.fori_loop(0, n, narrow, 0)
        back_recv[k, me] = back_send[k, me]
        return carry

    def legendre_and_return(k, carry):
        legendre(k, carry)
        exchange(back_send, back_recv, back_send_sem, back_recv_sem, k)
        return carry

    lax.fori_loop(0, last, legendre_and_return, 0)
    legendre(last, 0)
    parts = ((0, early), (early, slots - early))
    for i, part in enumerate(parts):
        exchange(back_send, back_recv, back_send_sem, back_recv_sem, last, part, last + i)

    def spread(k, s):
        flat[pl.ds(0, 2 * quads), :] = (
            back_recv[k, :, s].astype(F32).reshape(2 * quads, LANES)
        )
        both = [flat[pl.ds(h, quads, stride=2), :].astype(BF16) for h in range(2)]
        return jnp.concatenate(both, axis=1)

    for k in range(last):
        wait_for(others(back_recv, k), back_recv_sem.at[k])

        def add(s, carry, k=k):
            part = dot(table[k], spread(k, s), (0, 0))
            acc[s] = part if k == 0 else part + acc[s]
            return carry

        lax.fori_loop(0, slots, add, 0)

    def finish(s, carry):
        total = dot(turned[...], spread(last, s)) + acc[s]
        for h in range(2):
            out[s, h * half_points : (h + 1) * half_points, :] = total[
                h * padded_half : h * padded_half + half_points
            ].astype(BF16)
        return carry

    def piece(buffer, part):
        return buffer.at[last, pl.ds(0, n - 1), pl.ds(*part)]

    for k in range(chunks):
        wait_for(others(send, k), send_sem.at[k])
    for k in range(last):
        wait_for(others(back_send, k), back_send_sem.at[k])
    wait_for(stat_recv.at[pl.ds(0, block - 1)], stat_sems.at[0])
    wait_for(block_recv.at[pl.ds(0, chips // block - 1)], block_sems.at[0])
    for i, (first_slot, size) in enumerate(parts):
        wait_for(piece(back_recv, parts[i]), back_recv_sem.at[last + i])
        lax.fori_loop(first_slot, first_slot + size, finish, 0)
    for i, part in enumerate(parts):
        wait_for(piece(back_send, part), back_send_sem.at[last + i])


def wave_rows(wave_count, longitudes, padded_half):
    half = longitudes // 2
    number = np.arange(wave_count)
    phase = number[:, None] * np.arange(half)[None, :] % longitudes
    angle = phase * (2.0 * math.pi / longitudes)
    sine = np.where(number[:, None] > 0, -np.sin(angle), np.cos(angle))
    rows = np.zeros((wave_count, 2, padded_half + LANES), np.float32)
    rows[:, :, :half] = np.stack([np.cos(angle), sine], axis=1) / math.sqrt(longitudes)
    rows[:, :, padded_half] = 1.0 - 2.0 * (number % 2)[:, None]
    rows[0, 1, padded_half + 1] = 1.0
    return jnp.asarray(rows.reshape(2 * wave_count, -1), BF16)


def body(
    grid_values, lat_counts, owner_wavenumber, legendre, quad_weight, spectral_gain, channel_mix
):
    slots, longitudes, channels = grid_values.shape
    n = lat_counts.shape[0]
    share, live_total, degrees = legendre.shape
    chunks = share // PAIR
    padded_half = -(-longitudes // (2 * 256)) * 256
    padded_points = 2 * padded_half
    quads = n * PAIR * 2
    rows = n * slots
    waves = wave_rows(owner_wavenumber.shape[0], longitudes, padded_half)
    smem = pl.BlockSpec(memory_space=pltpu.SMEM)
    anywhere = pl.BlockSpec(memory_space=pl.ANY)
    message = (chunks, n, slots, ROWS, LANES)
    dma = pltpu.SemaphoreType.DMA
    block = 4 if n // 2 % 4 == 0 else 1
    dims = (n, slots, longitudes, chunks, live_total * longitudes)
    return pl.pallas_call(
        functools.partial(kernel, dims),
        out_shape=pltpu.VMEM(grid_values.shape, BF16),
        in_specs=[smem, smem] + [anywhere] * 8,
        out_specs=pl.BlockSpec(memory_space=pltpu.VMEM),
        scratch_shapes=[
            pltpu.VMEM((slots, padded_points, channels), BF16),
            pltpu.VMEM(waves.shape, BF16),
            pltpu.VMEM((share, live_total, degrees), BF16),
            pltpu.VMEM((owner_wavenumber.shape[0] // LANES, LANES), jnp.int32),
            pltpu.VMEM((1, n), jnp.int32),
            pltpu.VMEM((live_total // LANES, LANES), F32),
            pltpu.VMEM((degrees, channels), F32),
            pltpu.VMEM((channels, channels), BF16),
            pltpu.VMEM((chunks, quads, padded_points), BF16),
            pltpu.VMEM((padded_points, quads), BF16),
            pltpu.VMEM((slots, padded_points, channels), F32),
            pltpu.VMEM(message, BF16),
            pltpu.VMEM(message, BF16),
            pltpu.VMEM(message, BF16),
            pltpu.VMEM(message, BF16),
            pltpu.VMEM((max(rows * ROWS, 2 * quads), LANES), F32),
            pltpu.VMEM((rows, 2 * channels), BF16),
            pltpu.VMEM((share, rows, degrees), BF16),
            pltpu.VMEM((rows, LANES), F32),
            pltpu.VMEM((chunks * quads, LANES), F32),
            pltpu.VMEM((degrees, 2 * channels), BF16),
            pltpu.VMEM((2, 2, LANES), F32),
            pltpu.VMEM((2, LANES), F32),
            pltpu.VMEM((2, LANES), F32),
            pltpu.VMEM((block, 2, LANES), F32),
            pltpu.VMEM((2, LANES), F32),
            pltpu.VMEM((n // 2 // block, 2, LANES), F32),
            pltpu.VMEM((2, 2, LANES), F32),
            dma((slots, 2)),
            dma((7,)),
            dma((chunks,)),
            dma((chunks,)),
            dma((chunks + 1,)),
            dma((chunks + 1,)),
            dma((2,)),
            dma((2,)),
            dma((2,)),
            dma((2,)),
            pltpu.SemaphoreType.REGULAR,
        ],
        compiler_params=pltpu.CompilerParams(
            collective_id=0, has_side_effects=True, vmem_limit_bytes=54 * 1024 * 1024
        ),
    )(
        lat_counts,
        owner_wavenumber,
        grid_values,
        waves,
        legendre,
        owner_wavenumber.reshape(-1, LANES),
        lat_counts[None, :],
        quad_weight.reshape(-1, LANES),
        spectral_gain,
        channel_mix,
    )


def solution(mesh):
    return jax.shard_map(
        body,
        mesh=mesh,
        in_specs=(P(("group", "lat"), None, None), P(), P(), P("lat", None, None), P(), P(), P()),
        out_specs=P(("group", "lat"), None, None),
        check_vma=False,
    )
```

```python
import functools
import math

import jax
import jax.numpy as jnp
import numpy as np
from jax import lax
from jax.experimental import pallas as pl
from jax.experimental.pallas import tpu as pltpu
from jax.sharding import PartitionSpec as P

MESH = pl.DeviceIdType.MESH
LANES = 128
PAIR = 2
ROWS = 8
BF16, F32 = jnp.bfloat16, jnp.float32


def dot(a, b, contract=(1, 0)):
    return lax.dot_general(
        a, b, (((contract[0],), (contract[1],)), ((), ())), preferred_element_type=F32
    )


def kernel(
    dims,
    x_hbm,
    waves_hbm,
    leg_hbm,
    number_hbm,
    count_hbm,
    quad_hbm,
    gain_hbm,
    mix_hbm,
    out,
    x,
    waves,
    leg,
    number_row,
    count_row,
    quad,
    gain,
    mix,
    table,
    turned,
    acc,
    send,
    recv,
    back_send,
    back_recv,
    flat,
    weighted,
    padded,
    row_weight,
    table_sum,
    mixed,
    stat_mine,
    stat_pair,
    stat_send,
    stat_recv,
    block_send,
    block_recv,
    stat_total,
    x_sem,
    load_sem,
    send_sem,
    recv_sem,
    back_send_sem,
    back_recv_sem,
    pair_sems,
    stat_sems,
    block_sems,
    total_sems,
    far_sem,
):
    n, slots, longitudes, chunks, points = dims
    me = lax.axis_index("lat")
    quads = n * PAIR * 2
    half_points = longitudes // 2
    padded_half = table.shape[2] // 2
    padded_points = 2 * padded_half
    degrees = gain.shape[0]
    chips, chip, core = n // 2, me // 2, lax.rem(me, 2)
    partner = me + 1 - 2 * core
    last = chunks - 1
    early = slots - 1

    def ring(here, size, step):
        far = size - step
        half = (far + 1) // 2
        return lax.rem(here + half * (1 - 2 * lax.rem(far + 1, 2)) + size, size)

    def peer_of(step):
        return ring(me, n, step)

    barrier = pltpu.get_barrier_semaphore()
    near_from = n - n // 2

    def greet(step, carry):
        pl.semaphore_signal(
            barrier, inc=1, device_id={"lat": peer_of(step)}, device_id_type=MESH
        )
        return carry

    lax.fori_loop(near_from, n, greet, 0)

    loads = [
        pltpu.make_async_copy(source, target, load_sem.at[i])
        for i, (source, target) in enumerate(
            (
                (number_hbm, number_row),
                (waves_hbm, waves),
                (count_hbm, count_row),
                (leg_hbm, leg),
                (quad_hbm, quad),
                (gain_hbm, gain),
                (mix_hbm, mix),
            )
        )
    ]

    def x_copy(s, h):
        return pltpu.make_async_copy(
            x_hbm.at[s, pl.ds(h * half_points, half_points)],
            x.at[s, pl.ds(h * padded_half, half_points)],
            x_sem.at[s, h],
        )

    halves = [(s, h) for s in range(slots) for h in range(2)]
    for load in loads[:2]:
        load.start()
    for s, h in halves:
        x_copy(s, h).start()
    for load in loads[2:]:
        load.start()

    if padded_half > half_points:
        for h in range(2):
            x[:, h * padded_half + half_points : (h + 1) * padded_half, :] = jnp.zeros(
                (slots, padded_half - half_points, x.shape[2]), BF16
            )
    for load in loads[:2]:
        load.wait()

    def build(k):
        q, r = (lax.broadcasted_iota(jnp.int32, (quads, LANES), i) for i in range(2))
        slot = (q // (2 * PAIR)) * (chunks * PAIR) + k * PAIR + lax.rem(q // 2, PAIR)
        held = jnp.zeros((quads, LANES), F32)
        for i in range(number_row.shape[0]):
            numbers = number_row[i : i + 1, :].astype(F32)
            held = held + jnp.where(slot == r + i * LANES, numbers, 0.0)
        part = lax.rem(lax.broadcasted_iota(jnp.int32, (quads, 1), 0), 2).astype(F32)
        code = 2.0 * jnp.sum(held, axis=1, keepdims=True) + part
        column = lax.broadcasted_iota(jnp.int32, (quads, waves.shape[0]), 1).astype(F32)
        hot = jnp.where(column == code, 1.0, 0.0).astype(F32).astype(BF16)
        rows = dot(hot, waves[...])
        first, sign = rows[:, :padded_half], rows[:, padded_half : padded_half + 1]
        table[k, :, :padded_half] = first.astype(BF16)
        table[k, :, padded_half:] = (first * sign).astype(BF16)
        return rows[:, padded_half + 1 : padded_half + 2]

    def fourier(k):
        residual = build(k)

        def one(s, carry):
            if k == 0:
                for h in range(2):
                    x_copy(s, h).wait()
            values = dot(table[k], x[s])
            values = values - residual * values.astype(BF16).astype(F32)
            flat[pl.ds(0, quads, stride=2), :] = values[:, :LANES]
            flat[pl.ds(1, quads, stride=2), :] = values[:, LANES:]
            send[k, :, s] = (
                flat[pl.ds(0, 2 * quads), :].reshape(n, ROWS, LANES).astype(BF16)
            )
            return carry

        cut = slots - 2 if k == 0 else slots
        lax.fori_loop(0, cut, one, 0)
        if k == 0:
            pl.semaphore_wait(barrier, n // 2)
            for edge in (n // 4, n - n // 4):
                pl.semaphore_signal(
                    far_sem, inc=1, device_id={"lat": lax.rem(me + edge, n)}, device_id_type=MESH
                )
        lax.fori_loop(cut, slots, one, 0)
        recv[k, me] = send[k, me]

    def exchange(source, target, send_sems, recv_sems, k, parts=None, only=None, steps=(1, n)):
        def cut(ref, i, part):
            return ref.at[k, i] if part is None else ref.at[k, i, pl.ds(*part)]

        def one(step, carry):
            peer = peer_of(step)

            def send_to_peer():
                for at, part in parts or ((k, None),):
                    pltpu.make_async_remote_copy(
                        cut(source, peer, part),
                        cut(target, me, part),
                        send_sems.at[at],
                        recv_sems.at[at],
                        device_id={"lat": peer},
                        device_id_type=MESH,
                    ).start()

            if only is None:
                send_to_peer()
            else:
                pl.when(only(peer))(send_to_peer)
            return carry

        lax.fori_loop(*steps, one, 0)

    def wait_for(buffer, sem):
        pltpu.make_async_copy(buffer, buffer, sem).wait()

    def others(buffer, k):
        return buffer.at[k, pl.ds(0, n - 1)]

    fourier(0)
    exchange(send, recv, send_sem, recv_sem, 0, steps=(near_from, n))
    pl.semaphore_wait(far_sem, 2)
    exchange(send, recv, send_sem, recv_sem, 0, steps=(1, near_from))

    def entry(row, at):
        lane = lax.broadcasted_iota(jnp.int32, row.shape, 1)
        chosen = jnp.where(lane == at, row.astype(F32), 0.0)
        return jnp.sum(chosen, axis=1, keepdims=True)

    loads[2].wait()
    live = entry(count_row[...], me)
    step_rows = 96

    def sums(i, carry):
        first, second = carry
        s = i // (padded_points // step_rows)
        r = pl.multiple_of(lax.rem(i, padded_points // step_rows) * step_rows, step_rows)
        on = jnp.where(lax.convert_element_type(s, F32) < live, 1.0, 0.0).astype(F32)
        values = x[s, pl.ds(r, step_rows), :].astype(F32) * on
        values = values.reshape(step_rows // 8, 8, values.shape[1])
        return first + jnp.sum(values, axis=0), second + jnp.sum(values * values, axis=0)

    zero = jnp.zeros((8, x.shape[2]), F32)
    first, second = lax.fori_loop(
        0, slots * (padded_points // step_rows), sums, (zero, zero)
    )
    first = jnp.sum(first, axis=0, keepdims=True)
    second = jnp.sum(second, axis=0, keepdims=True)
    for i, part in enumerate((first, second)):
        for h in range(2):
            stat_mine[i, h : h + 1, :] = part[:, h * LANES : (h + 1) * LANES]

    def pair_copy(source, target, sems):
        return pltpu.make_async_remote_copy(
            source, target, sems.at[0], sems.at[1], device_id={"lat": partner}, device_id_type=MESH
        )

    block = stat_recv.shape[0]
    rank, lane = chip // block, lax.rem(chip, block)

    def stat_copies(source, target, here, size, chip_of, sems):
        def one(step, carry):
            pltpu.make_async_remote_copy(
                source,
                target.at[here],
                sems.at[0],
                sems.at[1],
                device_id={"lat": chip_of(ring(here, size, step)) * 2 + core},
                device_id_type=MESH,
            ).start()
            return carry

        lax.fori_loop(1, size, one, 0)

    to_partner = pair_copy(stat_mine.at[1 - core], stat_pair, pair_sems)
    to_partner.start()
    for k in range(1, chunks):
        fourier(k)
        if k == 1:
            to_partner.wait()
            stat_send[...] = stat_mine[core] + stat_pair[...]
            stat_recv[lane] = stat_send[...]
            stat_copies(stat_send, stat_recv, lane, block, lambda i: rank * block + i, stat_sems)
        if k == last:
            wait_for(stat_recv.at[pl.ds(0, block - 1)], stat_sems.at[1])
            block_send[...] = jnp.sum(stat_recv[...], axis=0)
            block_recv[rank] = block_send[...]
            stat_copies(
                block_send, block_recv, rank, chips // block, lambda i: i * block + lane, block_sems
            )
        exchange(send, recv, send_sem, recv_sem, k)

    for load in loads[3:]:
        load.wait()
    row = lax.broadcasted_iota(jnp.int32, (n * slots, n), 0)
    device = lax.broadcasted_iota(jnp.int32, (n * slots, n), 1)
    holder, slot_no = row // slots, lax.rem(row[:, :1], slots).astype(F32)
    number_live = count_row[...].astype(F32)
    start = jnp.sum(jnp.where(device < holder, number_live, 0.0), axis=1, keepdims=True)
    count = jnp.sum(jnp.where(device == holder, number_live, 0.0), axis=1, keepdims=True)
    latitude = lax.broadcasted_iota(jnp.int32, (n * slots, leg.shape[1]), 1).astype(F32)
    hot = (latitude == start + slot_no) & (slot_no < count)
    hot = jnp.where(hot, 1.0, 0.0).astype(F32)
    held = jnp.zeros(row_weight.shape, F32)
    for i in range(quad.shape[0]):
        held = held + hot[:, i * LANES : (i + 1) * LANES] * quad[i : i + 1, :]
    row_weight[...] = jnp.broadcast_to(
        jnp.sum(held, axis=1, keepdims=True), row_weight.shape
    )
    pick = hot.astype(BF16)

    def pad(w, carry):
        padded[w] = dot(pick, leg[w]).astype(BF16)
        return carry

    lax.fori_loop(0, chunks * PAIR, pad, 0)

    point = lax.rem(lax.broadcasted_iota(jnp.int32, (padded_points, LANES), 0), padded_half)
    ones = jnp.where(point < half_points, 1.0, 0.0).astype(F32).astype(BF16)

    def sum_table(k, carry):
        table_sum[pl.ds(pl.multiple_of(k * quads, quads), quads), :] = dot(table[k], ones)
        return carry

    lax.fori_loop(0, chunks, sum_table, 0)
    r, c = (lax.broadcasted_iota(jnp.int32, (quads, quads), i) for i in range(2))
    unit = jnp.where(r == c, 1.0, 0.0).astype(F32).astype(BF16)
    turned[...] = dot(table[last], unit, (0, 0)).astype(BF16)

    wait_for(block_recv.at[pl.ds(0, chips // block - 1)], block_sems.at[1])
    stat_total[core] = jnp.sum(block_recv[...], axis=0)
    total_copy = pair_copy(stat_total.at[core], stat_total.at[core], total_sems)
    total_copy.start()
    total_copy.wait()
    mean = stat_total[0] / points
    variance = stat_total[1] / points - mean * mean
    scale = lax.rsqrt(variance + 1e-05)

    rows = n * slots

    def legendre(k, carry):
        wait_for(others(recv, k), recv_sem.at[k])

        def widen(i, inner):
            at = pl.multiple_of(i * slots * ROWS, ROWS)
            flat[pl.ds(at, slots * ROWS), :] = (
                recv[k, i].astype(F32).reshape(slots * ROWS, LANES)
            )
            return inner

        lax.fori_loop(0, n, widen, 0)

        def wave(w, inner):
            wave_slot = me * chunks * PAIR + k * PAIR + w
            number = jnp.zeros((1, 1), F32)
            for i in range(number_row.shape[0]):
                number = number + entry(number_row[i : i + 1, :], wave_slot - i * LANES)
            is_zero = jnp.where(number == 0.0, 1.0, 0.0).astype(F32)
            for h in range(2):
                m_h, s_h = mean[h : h + 1], scale[h : h + 1]
                re = flat[pl.ds(w * 4 + h, rows, stride=ROWS), :]
                im = flat[pl.ds(w * 4 + 2 + h, rows, stride=ROWS), :]
                re = re + is_zero * im
                im = im - is_zero * im
                at = k * quads + me * 2 * PAIR + w * 2
                d_re = table_sum[pl.ds(at, 1), :]
                d_im = table_sum[pl.ds(at + 1, 1), :] * (1.0 - is_zero)
                for t, (value, d) in enumerate(((re, d_re), (im, d_im))):
                    left = (2 * t + h) * LANES
                    weighted[:, left : left + LANES] = (
                        ((value - m_h * d) * s_h) * row_weight[...]
                    ).astype(BF16)
            here = padded[k * PAIR + w]
            coefficient = dot(here, weighted[...], (0, 0))
            keep = lax.broadcasted_iota(jnp.int32, (degrees, 1), 0).astype(F32) >= number
            factor = jnp.where(keep, gain[...], 0.0)
            for t in range(2):
                cols = slice(2 * t * LANES, 2 * (t + 1) * LANES)
                filtered = (coefficient[:, cols] * factor).astype(BF16)
                mixed[:, cols] = dot(filtered, mix[...]).astype(BF16)
            synthesis = dot(here, mixed[...])
            for t in range(2):
                doubled = 2.0 - is_zero if t == 0 else 2.0 - 2.0 * is_zero
                for h in range(2):
                    left = (2 * t + h) * LANES
                    flat[pl.ds(w * 4 + t * 2 + h, rows, stride=ROWS), :] = (
                        synthesis[:, left : left + LANES] * doubled
                    )
            return inner

        lax.fori_loop(0, PAIR, wave, 0)

        def narrow(i, inner):
            at = pl.multiple_of(i * slots * ROWS, ROWS)
            back_send[k, i] = (
                flat[pl.ds(at, slots * ROWS), :].reshape(slots, ROWS, LANES).astype(BF16)
            )
            return inner

        lax.fori_loop(0, n, narrow, 0)
        back_recv[k, me] = back_send[k, me]
        return carry

    def legendre_and_return(k, carry):
        legendre(k, carry)
        exchange(back_send, back_recv, back_send_sem, back_recv_sem, k)
        return carry

    lax.fori_loop(0, last, legendre_and_return, 0)
    legendre(last, 0)
    parts = ((0, early), (early, slots - early))
    named = [(last + i, part) for i, part in enumerate(parts)]
    for some, only in (
        (named, lambda peer: peer < n // 2),
        (named[:1], lambda peer: peer >= n // 2),
        (named[1:], lambda peer: peer >= n // 2),
    ):
        exchange(back_send, back_recv, back_send_sem, back_recv_sem, last, some, only)

    def spread(k, s):
        flat[pl.ds(0, 2 * quads), :] = (
            back_recv[k, :, s].astype(F32).reshape(2 * quads, LANES)
        )
        both = [flat[pl.ds(h, quads, stride=2), :].astype(BF16) for h in range(2)]
        return jnp.concatenate(both, axis=1)

    for k in range(last):
        wait_for(others(back_recv, k), back_recv_sem.at[k])

        def add(s, carry, k=k):
            part = dot(table[k], spread(k, s), (0, 0))
            acc[s] = part if k == 0 else part + acc[s]
            return carry

        lax.fori_loop(0, slots, add, 0)

    def finish(s, carry):
        total = dot(turned[...], spread(last, s)) + acc[s]
        for h in range(2):
            out[s, h * half_points : (h + 1) * half_points, :] = total[
                h * padded_half : h * padded_half + half_points
            ].astype(BF16)
        return carry

    def piece(buffer, part):
        return buffer.at[last, pl.ds(0, n - 1), pl.ds(*part)]

    for k in range(chunks):
        wait_for(others(send, k), send_sem.at[k])
    for k in range(last):
        wait_for(others(back_send, k), back_send_sem.at[k])
    wait_for(stat_recv.at[pl.ds(0, block - 1)], stat_sems.at[0])
    wait_for(block_recv.at[pl.ds(0, chips // block - 1)], block_sems.at[0])
    for i, (first_slot, size) in enumerate(parts):
        wait_for(piece(back_recv, parts[i]), back_recv_sem.at[last + i])
        lax.fori_loop(first_slot, first_slot + size, finish, 0)
    for i, part in enumerate(parts):
        wait_for(piece(back_send, part), back_send_sem.at[last + i])


def wave_rows(wave_count, longitudes, padded_half):
    half = longitudes // 2
    number = np.arange(wave_count)
    phase = number[:, None] * np.arange(half)[None, :] % longitudes
    angle = phase * (2.0 * math.pi / longitudes)
    sine = np.where(number[:, None] > 0, -np.sin(angle), np.cos(angle))
    rows = np.zeros((wave_count, 2, padded_half + LANES), np.float32)
    rows[:, :, :half] = np.stack([np.cos(angle), sine], axis=1) / math.sqrt(longitudes)
    rows[:, :, padded_half] = 1.0 - 2.0 * (number % 2)[:, None]
    rows[0, 1, padded_half + 1] = 1.0
    return jnp.asarray(rows.reshape(2 * wave_count, -1), BF16)


def body(
    grid_values, lat_counts, owner_wavenumber, legendre, quad_weight, spectral_gain, channel_mix
):
    slots, longitudes, channels = grid_values.shape
    n = lat_counts.shape[0]
    share, live_total, degrees = legendre.shape
    chunks = share // PAIR
    padded_half = -(-longitudes // (2 * 256)) * 256
    padded_points = 2 * padded_half
    quads = n * PAIR * 2
    rows = n * slots
    waves = wave_rows(owner_wavenumber.shape[0], longitudes, padded_half)
    anywhere = pl.BlockSpec(memory_space=pl.ANY)
    message = (chunks, n, slots, ROWS, LANES)
    dma = pltpu.SemaphoreType.DMA
    block = 4 if n // 2 % 4 == 0 else 1
    dims = (n, slots, longitudes, chunks, live_total * longitudes)
    return pl.pallas_call(
        functools.partial(kernel, dims),
        out_shape=pltpu.VMEM(grid_values.shape, BF16),
        in_specs=[anywhere] * 8,
        out_specs=pl.BlockSpec(memory_space=pltpu.VMEM),
        scratch_shapes=[
            pltpu.VMEM((slots, padded_points, channels), BF16),
            pltpu.VMEM(waves.shape, BF16),
            pltpu.VMEM((share, live_total, degrees), BF16),
            pltpu.VMEM((owner_wavenumber.shape[0] // LANES, LANES), jnp.int32),
            pltpu.VMEM((1, n), jnp.int32),
            pltpu.VMEM((live_total // LANES, LANES), F32),
            pltpu.VMEM((degrees, channels), F32),
            pltpu.VMEM((channels, channels), BF16),
            pltpu.VMEM((chunks, quads, padded_points), BF16),
            pltpu.VMEM((padded_points, quads), BF16),
            pltpu.VMEM((slots, padded_points, channels), F32),
            pltpu.VMEM(message, BF16),
            pltpu.VMEM(message, BF16),
            pltpu.VMEM(message, BF16),
            pltpu.VMEM(message, BF16),
            pltpu.VMEM((max(rows * ROWS, 2 * quads), LANES), F32),
            pltpu.VMEM((rows, 2 * channels), BF16),
            pltpu.VMEM((share, rows, degrees), BF16),
            pltpu.VMEM((rows, LANES), F32),
            pltpu.VMEM((chunks * quads, LANES), F32),
            pltpu.VMEM((degrees, 2 * channels), BF16),
            pltpu.VMEM((2, 2, LANES), F32),
            pltpu.VMEM((2, LANES), F32),
            pltpu.VMEM((2, LANES), F32),
            pltpu.VMEM((block, 2, LANES), F32),
            pltpu.VMEM((2, LANES), F32),
            pltpu.VMEM((n // 2 // block, 2, LANES), F32),
            pltpu.VMEM((2, 2, LANES), F32),
            dma((slots, 2)),
            dma((7,)),
            dma((chunks,)),
            dma((chunks,)),
            dma((chunks + 1,)),
            dma((chunks + 1,)),
            dma((2,)),
            dma((2,)),
            dma((2,)),
            dma((2,)),
            pltpu.SemaphoreType.REGULAR,
        ],
        compiler_params=pltpu.CompilerParams(
            collective_id=0, has_side_effects=True, vmem_limit_bytes=54 * 1024 * 1024
        ),
    )(
        grid_values,
        waves,
        legendre,
        owner_wavenumber.reshape(-1, LANES),
        lat_counts[None, :],
        quad_weight.reshape(-1, LANES),
        spectral_gain,
        channel_mix,
    )


def solution(mesh):
    return jax.shard_map(
        body,
        mesh=mesh,
        in_specs=(P(("group", "lat"), None, None), P(), P(), P("lat", None, None), P(), P(), P()),
        out_specs=P(("group", "lat"), None, None),
        check_vma=False,
    )
```

```python
import functools
import math

import jax
import jax.numpy as jnp
import numpy as np
from jax import lax
from jax.experimental import pallas as pl
from jax.experimental.pallas import tpu as pltpu
from jax.sharding import PartitionSpec as P

MESH = pl.DeviceIdType.MESH
LANES = 128
PAIR = 2
ROWS = 8
BF16, F32 = jnp.bfloat16, jnp.float32


def dot(a, b, contract=(1, 0)):
    return lax.dot_general(
        a, b, (((contract[0],), (contract[1],)), ((), ())), preferred_element_type=F32
    )


def kernel(
    dims,
    x_hbm,
    waves_hbm,
    leg_hbm,
    number_hbm,
    count_hbm,
    quad_hbm,
    gain_hbm,
    mix_hbm,
    out,
    x,
    waves,
    leg,
    number_row,
    count_row,
    quad,
    gain,
    mix,
    table,
    turned,
    acc,
    send,
    recv,
    back_send,
    back_recv,
    flat,
    weighted,
    padded,
    row_weight,
    table_sum,
    mixed,
    stat_mine,
    stat_pair,
    stat_send,
    stat_recv,
    block_send,
    block_recv,
    stat_total,
    x_sem,
    load_sem,
    send_sem,
    recv_sem,
    back_send_sem,
    back_recv_sem,
    pair_sems,
    stat_sems,
    block_sems,
    total_sems,
    far_sem,
):
    n, slots, longitudes, chunks, points = dims
    me = lax.axis_index("lat")
    quads = n * PAIR * 2
    half_points = longitudes // 2
    padded_half = table.shape[2] // 2
    padded_points = 2 * padded_half
    degrees = gain.shape[0]
    chips, chip, core = n // 2, me // 2, lax.rem(me, 2)
    partner = me + 1 - 2 * core
    last = chunks - 1
    early = slots - 1

    def ring(here, size, step):
        far = size - step
        half = (far + 1) // 2
        return lax.rem(here + half * (1 - 2 * lax.rem(far + 1, 2)) + size, size)

    def peer_of(step):
        return ring(me, n, step)

    barrier = pltpu.get_barrier_semaphore()
    near_from = n - n // 2

    def greet(step, carry):
        pl.semaphore_signal(
            barrier, inc=1, device_id={"lat": peer_of(step)}, device_id_type=MESH
        )
        return carry

    lax.fori_loop(near_from, n, greet, 0)

    loads = [
        pltpu.make_async_copy(source, target, load_sem.at[i])
        for i, (source, target) in enumerate(
            (
                (number_hbm, number_row),
                (waves_hbm, waves),
                (count_hbm, count_row),
                (leg_hbm, leg),
                (quad_hbm, quad),
                (gain_hbm, gain),
                (mix_hbm, mix),
            )
        )
    ]

    def x_copy(s, h):
        return pltpu.make_async_copy(
            x_hbm.at[s, pl.ds(h * half_points, half_points)],
            x.at[s, pl.ds(h * padded_half, half_points)],
            x_sem.at[s, h],
        )

    halves = [(s, h) for s in range(slots) for h in range(2)]
    for load in loads[:2]:
        load.start()
    for s, h in halves:
        x_copy(s, h).start()
    for load in loads[2:]:
        load.start()

    if padded_half > half_points:
        for h in range(2):
            x[:, h * padded_half + half_points : (h + 1) * padded_half, :] = jnp.zeros(
                (slots, padded_half - half_points, x.shape[2]), BF16
            )
    for load in loads[:2]:
        load.wait()

    def build(k):
        q, r = (lax.broadcasted_iota(jnp.int32, (quads, LANES), i) for i in range(2))
        slot = (q // (2 * PAIR)) * (chunks * PAIR) + k * PAIR + lax.rem(q // 2, PAIR)
        held = jnp.zeros((quads, LANES), F32)
        for i in range(number_row.shape[0]):
            numbers = number_row[i : i + 1, :].astype(F32)
            held = held + jnp.where(slot == r + i * LANES, numbers, 0.0)
        part = lax.rem(lax.broadcasted_iota(jnp.int32, (quads, 1), 0), 2).astype(F32)
        code = 2.0 * jnp.sum(held, axis=1, keepdims=True) + part
        column = lax.broadcasted_iota(jnp.int32, (quads, waves.shape[0]), 1).astype(F32)
        hot = jnp.where(column == code, 1.0, 0.0).astype(F32).astype(BF16)
        rows = dot(hot, waves[...])
        first, sign = rows[:, :padded_half], rows[:, padded_half : padded_half + 1]
        table[k, :, :padded_half] = first.astype(BF16)
        table[k, :, padded_half:] = (first * sign).astype(BF16)
        return rows[:, padded_half + 1 : padded_half + 2]

    def fourier(k):
        residual = build(k)

        def one(s, carry):
            if k == 0:
                for h in range(2):
                    x_copy(s, h).wait()
            values = dot(table[k], x[s])
            values = values - residual * values.astype(BF16).astype(F32)
            flat[pl.ds(0, quads, stride=2), :] = values[:, :LANES]
            flat[pl.ds(1, quads, stride=2), :] = values[:, LANES:]
            send[k, :, s] = (
                flat[pl.ds(0, 2 * quads), :].reshape(n, ROWS, LANES).astype(BF16)
            )
            return carry

        cut = slots - 2 if k == 0 else slots
        lax.fori_loop(0, cut, one, 0)
        if k == 0:
            pl.semaphore_wait(barrier, n // 2)
            for edge in (n // 4, n - n // 4):
                pl.semaphore_signal(
                    far_sem, inc=1, device_id={"lat": lax.rem(me + edge, n)}, device_id_type=MESH
                )
        lax.fori_loop(cut, slots, one, 0)
        recv[k, me] = send[k, me]

    def exchange(source, target, send_sems, recv_sems, k, parts=None, only=None, steps=(1, n)):
        def cut(ref, i, part):
            return ref.at[k, i] if part is None else ref.at[k, i, pl.ds(*part)]

        def one(step, carry):
            peer = peer_of(step)

            def send_to_peer():
                for at, part in parts or ((k, None),):
                    pltpu.make_async_remote_copy(
                        cut(source, peer, part),
                        cut(target, me, part),
                        send_sems.at[at],
                        recv_sems.at[at],
                        device_id={"lat": peer},
                        device_id_type=MESH,
                    ).start()

            if only is None:
                send_to_peer()
            else:
                pl.when(only(peer))(send_to_peer)
            return carry

        lax.fori_loop(*steps, one, 0)

    def wait_for(buffer, sem):
        pltpu.make_async_copy(buffer, buffer, sem).wait()

    def others(buffer, k):
        return buffer.at[k, pl.ds(0, n - 1)]

    fourier(0)
    exchange(send, recv, send_sem, recv_sem, 0, steps=(near_from, n))
    pl.semaphore_wait(far_sem, 2)
    exchange(send, recv, send_sem, recv_sem, 0, steps=(1, near_from))

    def entry(row, at):
        lane = lax.broadcasted_iota(jnp.int32, row.shape, 1)
        chosen = jnp.where(lane == at, row.astype(F32), 0.0)
        return jnp.sum(chosen, axis=1, keepdims=True)

    loads[2].wait()
    live = entry(count_row[...], me)
    step_rows = 96

    def sums(i, carry):
        first, second = carry
        s = i // (padded_points // step_rows)
        r = pl.multiple_of(lax.rem(i, padded_points // step_rows) * step_rows, step_rows)
        on = jnp.where(lax.convert_element_type(s, F32) < live, 1.0, 0.0).astype(F32)
        values = x[s, pl.ds(r, step_rows), :].astype(F32) * on
        values = values.reshape(step_rows // 8, 8, values.shape[1])
        return first + jnp.sum(values, axis=0), second + jnp.sum(values * values, axis=0)

    zero = jnp.zeros((8, x.shape[2]), F32)
    first, second = lax.fori_loop(
        0, slots * (padded_points // step_rows), sums, (zero, zero)
    )
    first = jnp.sum(first, axis=0, keepdims=True)
    second = jnp.sum(second, axis=0, keepdims=True)
    for i, part in enumerate((first, second)):
        for h in range(2):
            stat_mine[i, h : h + 1, :] = part[:, h * LANES : (h + 1) * LANES]

    def pair_copy(source, target, sems):
        return pltpu.make_async_remote_copy(
            source, target, sems.at[0], sems.at[1], device_id={"lat": partner}, device_id_type=MESH
        )

    block = stat_recv.shape[0]
    rank, lane = chip // block, lax.rem(chip, block)

    def stat_copies(source, target, here, size, chip_of, sems):
        def one(step, carry):
            pltpu.make_async_remote_copy(
                source,
                target.at[here],
                sems.at[0],
                sems.at[1],
                device_id={"lat": chip_of(ring(here, size, step)) * 2 + core},
                device_id_type=MESH,
            ).start()
            return carry

        lax.fori_loop(1, size, one, 0)

    to_partner = pair_copy(stat_mine.at[1 - core], stat_pair, pair_sems)
    to_partner.start()
    for k in range(1, chunks):
        fourier(k)
        if k == 1:
            to_partner.wait()
            stat_send[...] = stat_mine[core] + stat_pair[...]
            stat_recv[lane] = stat_send[...]
            stat_copies(stat_send, stat_recv, lane, block, lambda i: rank * block + i, stat_sems)
        if k == last:
            wait_for(stat_recv.at[pl.ds(0, block - 1)], stat_sems.at[1])
            block_send[...] = jnp.sum(stat_recv[...], axis=0)
            block_recv[rank] = block_send[...]
            stat_copies(
                block_send, block_recv, rank, chips // block, lambda i: i * block + lane, block_sems
            )
        exchange(send, recv, send_sem, recv_sem, k)

    for load in loads[3:]:
        load.wait()
    row = lax.broadcasted_iota(jnp.int32, (n * slots, n), 0)
    device = lax.broadcasted_iota(jnp.int32, (n * slots, n), 1)
    holder, slot_no = row // slots, lax.rem(row[:, :1], slots).astype(F32)
    number_live = count_row[...].astype(F32)
    start = jnp.sum(jnp.where(device < holder, number_live, 0.0), axis=1, keepdims=True)
    count = jnp.sum(jnp.where(device == holder, number_live, 0.0), axis=1, keepdims=True)
    latitude = lax.broadcasted_iota(jnp.int32, (n * slots, leg.shape[1]), 1).astype(F32)
    hot = (latitude == start + slot_no) & (slot_no < count)
    hot = jnp.where(hot, 1.0, 0.0).astype(F32)
    held = jnp.zeros(row_weight.shape, F32)
    for i in range(quad.shape[0]):
        held = held + hot[:, i * LANES : (i + 1) * LANES] * quad[i : i + 1, :]
    row_weight[...] = jnp.broadcast_to(
        jnp.sum(held, axis=1, keepdims=True), row_weight.shape
    )
    pick = hot.astype(BF16)

    def pad(w, carry):
        padded[w] = dot(pick, leg[w]).astype(BF16)
        return carry

    lax.fori_loop(0, chunks * PAIR, pad, 0)

    point = lax.rem(lax.broadcasted_iota(jnp.int32, (padded_points, LANES), 0), padded_half)
    ones = jnp.where(point < half_points, 1.0, 0.0).astype(F32).astype(BF16)

    def sum_table(k, carry):
        table_sum[pl.ds(pl.multiple_of(k * quads, quads), quads), :] = dot(table[k], ones)
        return carry

    lax.fori_loop(0, chunks, sum_table, 0)
    r, c = (lax.broadcasted_iota(jnp.int32, (quads, quads), i) for i in range(2))
    unit = jnp.where(r == c, 1.0, 0.0).astype(F32).astype(BF16)
    turned[...] = dot(table[last], unit, (0, 0)).astype(BF16)

    wait_for(block_recv.at[pl.ds(0, chips // block - 1)], block_sems.at[1])
    stat_total[core] = jnp.sum(block_recv[...], axis=0)
    total_copy = pair_copy(stat_total.at[core], stat_total.at[core], total_sems)
    total_copy.start()
    total_copy.wait()
    mean = stat_total[0] / points
    variance = stat_total[1] / points - mean * mean
    scale = lax.rsqrt(variance + 1e-05)

    rows = n * slots

    def legendre(k, carry):
        wait_for(others(recv, k), recv_sem.at[k])

        def widen(i, inner):
            at = pl.multiple_of(i * slots * ROWS, ROWS)
            flat[pl.ds(at, slots * ROWS), :] = (
                recv[k, i].astype(F32).reshape(slots * ROWS, LANES)
            )
            return inner

        lax.fori_loop(0, n, widen, 0)

        def wave(w, inner):
            wave_slot = me * chunks * PAIR + k * PAIR + w
            number = jnp.zeros((1, 1), F32)
            for i in range(number_row.shape[0]):
                number = number + entry(number_row[i : i + 1, :], wave_slot - i * LANES)
            is_zero = jnp.where(number == 0.0, 1.0, 0.0).astype(F32)
            for h in range(2):
                m_h, s_h = mean[h : h + 1], scale[h : h + 1]
                re = flat[pl.ds(w * 4 + h, rows, stride=ROWS), :]
                im = flat[pl.ds(w * 4 + 2 + h, rows, stride=ROWS), :]
                re = re + is_zero * im
                im = im - is_zero * im
                at = k * quads + me * 2 * PAIR + w * 2
                d_re = table_sum[pl.ds(at, 1), :]
                d_im = table_sum[pl.ds(at + 1, 1), :] * (1.0 - is_zero)
                for t, (value, d) in enumerate(((re, d_re), (im, d_im))):
                    left = (2 * t + h) * LANES
                    weighted[:, left : left + LANES] = (
                        ((value - m_h * d) * s_h) * row_weight[...]
                    ).astype(BF16)
            here = padded[k * PAIR + w]
            coefficient = dot(here, weighted[...], (0, 0))
            keep = lax.broadcasted_iota(jnp.int32, (degrees, 1), 0).astype(F32) >= number
            factor = jnp.where(keep, gain[...], 0.0)
            for t in range(2):
                cols = slice(2 * t * LANES, 2 * (t + 1) * LANES)
                filtered = (coefficient[:, cols] * factor).astype(BF16)
                mixed[:, cols] = dot(filtered, mix[...]).astype(BF16)
            synthesis = dot(here, mixed[...])
            for t in range(2):
                doubled = 2.0 - is_zero if t == 0 else 2.0 - 2.0 * is_zero
                for h in range(2):
                    left = (2 * t + h) * LANES
                    flat[pl.ds(w * 4 + t * 2 + h, rows, stride=ROWS), :] = (
                        synthesis[:, left : left + LANES] * doubled
                    )
            return inner

        lax.fori_loop(0, PAIR, wave, 0)

        def narrow(i, inner):
            at = pl.multiple_of(i * slots * ROWS, ROWS)
            back_send[k, i] = (
                flat[pl.ds(at, slots * ROWS), :].reshape(slots, ROWS, LANES).astype(BF16)
            )
            return inner

        lax.fori_loop(0, n, narrow, 0)
        back_recv[k, me] = back_send[k, me]
        return carry

    def legendre_and_return(k, carry):
        legendre(k, carry)
        exchange(back_send, back_recv, back_send_sem, back_recv_sem, k)
        return carry

    lax.fori_loop(0, last, legendre_and_return, 0)
    legendre(last, 0)
    parts = ((0, early), (early, slots - early))
    named = [(last + i, part) for i, part in enumerate(parts)]

    def first_half(peer):
        return lax.rem(peer + 3 * n // 16, n) < n // 2

    def second_half(peer):
        return lax.rem(peer + 3 * n // 16, n) >= n // 2

    for some, only in ((named, first_half), (named[:1], second_half), (named[1:], second_half)):
        exchange(back_send, back_recv, back_send_sem, back_recv_sem, last, some, only)

    def spread(k, s):
        flat[pl.ds(0, 2 * quads), :] = (
            back_recv[k, :, s].astype(F32).reshape(2 * quads, LANES)
        )
        both = [flat[pl.ds(h, quads, stride=2), :].astype(BF16) for h in range(2)]
        return jnp.concatenate(both, axis=1)

    for k in range(last):
        wait_for(others(back_recv, k), back_recv_sem.at[k])

        def add(s, carry, k=k):
            part = dot(table[k], spread(k, s), (0, 0))
            acc[s] = part if k == 0 else part + acc[s]
            return carry

        lax.fori_loop(0, slots, add, 0)

    def finish(s, carry):
        total = dot(turned[...], spread(last, s)) + acc[s]
        for h in range(2):
            out[s, h * half_points : (h + 1) * half_points, :] = total[
                h * padded_half : h * padded_half + half_points
            ].astype(BF16)
        return carry

    def piece(buffer, part):
        return buffer.at[last, pl.ds(0, n - 1), pl.ds(*part)]

    for k in range(chunks):
        wait_for(others(send, k), send_sem.at[k])
    for k in range(last):
        wait_for(others(back_send, k), back_send_sem.at[k])
    wait_for(stat_recv.at[pl.ds(0, block - 1)], stat_sems.at[0])
    wait_for(block_recv.at[pl.ds(0, chips // block - 1)], block_sems.at[0])
    for i, (first_slot, size) in enumerate(parts):
        wait_for(piece(back_recv, parts[i]), back_recv_sem.at[last + i])
        lax.fori_loop(first_slot, first_slot + size, finish, 0)
    for i, part in enumerate(parts):
        wait_for(piece(back_send, part), back_send_sem.at[last + i])


def wave_rows(wave_count, longitudes, padded_half):
    half = longitudes // 2
    number = np.arange(wave_count)
    phase = number[:, None] * np.arange(half)[None, :] % longitudes
    angle = phase * (2.0 * math.pi / longitudes)
    sine = np.where(number[:, None] > 0, -np.sin(angle), np.cos(angle))
    rows = np.zeros((wave_count, 2, padded_half + LANES), np.float32)
    rows[:, :, :half] = np.stack([np.cos(angle), sine], axis=1) / math.sqrt(longitudes)
    rows[:, :, padded_half] = 1.0 - 2.0 * (number % 2)[:, None]
    rows[0, 1, padded_half + 1] = 1.0
    return jnp.asarray(rows.reshape(2 * wave_count, -1), BF16)


def body(
    grid_values, lat_counts, owner_wavenumber, legendre, quad_weight, spectral_gain, channel_mix
):
    slots, longitudes, channels = grid_values.shape
    n = lat_counts.shape[0]
    share, live_total, degrees = legendre.shape
    chunks = share // PAIR
    padded_half = -(-longitudes // (2 * 256)) * 256
    padded_points = 2 * padded_half
    quads = n * PAIR * 2
    rows = n * slots
    waves = wave_rows(owner_wavenumber.shape[0], longitudes, padded_half)
    anywhere = pl.BlockSpec(memory_space=pl.ANY)
    message = (chunks, n, slots, ROWS, LANES)
    dma = pltpu.SemaphoreType.DMA
    block = 4 if n // 2 % 4 == 0 else 1
    dims = (n, slots, longitudes, chunks, live_total * longitudes)
    return pl.pallas_call(
        functools.partial(kernel, dims),
        out_shape=pltpu.VMEM(grid_values.shape, BF16),
        in_specs=[anywhere] * 8,
        out_specs=pl.BlockSpec(memory_space=pltpu.VMEM),
        scratch_shapes=[
            pltpu.VMEM((slots, padded_points, channels), BF16),
            pltpu.VMEM(waves.shape, BF16),
            pltpu.VMEM((share, live_total, degrees), BF16),
            pltpu.VMEM((owner_wavenumber.shape[0] // LANES, LANES), jnp.int32),
            pltpu.VMEM((1, n), jnp.int32),
            pltpu.VMEM((live_total // LANES, LANES), F32),
            pltpu.VMEM((degrees, channels), F32),
            pltpu.VMEM((channels, channels), BF16),
            pltpu.VMEM((chunks, quads, padded_points), BF16),
            pltpu.VMEM((padded_points, quads), BF16),
            pltpu.VMEM((slots, padded_points, channels), F32),
            pltpu.VMEM(message, BF16),
            pltpu.VMEM(message, BF16),
            pltpu.VMEM(message, BF16),
            pltpu.VMEM(message, BF16),
            pltpu.VMEM((max(rows * ROWS, 2 * quads), LANES), F32),
            pltpu.VMEM((rows, 2 * channels), BF16),
            pltpu.VMEM((share, rows, degrees), BF16),
            pltpu.VMEM((rows, LANES), F32),
            pltpu.VMEM((chunks * quads, LANES), F32),
            pltpu.VMEM((degrees, 2 * channels), BF16),
            pltpu.VMEM((2, 2, LANES), F32),
            pltpu.VMEM((2, LANES), F32),
            pltpu.VMEM((2, LANES), F32),
            pltpu.VMEM((block, 2, LANES), F32),
            pltpu.VMEM((2, LANES), F32),
            pltpu.VMEM((n // 2 // block, 2, LANES), F32),
            pltpu.VMEM((2, 2, LANES), F32),
            dma((slots, 2)),
            dma((7,)),
            dma((chunks,)),
            dma((chunks,)),
            dma((chunks + 1,)),
            dma((chunks + 1,)),
            dma((2,)),
            dma((2,)),
            dma((2,)),
            dma((2,)),
            pltpu.SemaphoreType.REGULAR,
        ],
        compiler_params=pltpu.CompilerParams(
            collective_id=0, has_side_effects=True, vmem_limit_bytes=54 * 1024 * 1024
        ),
    )(
        grid_values,
        waves,
        legendre,
        owner_wavenumber.reshape(-1, LANES),
        lat_counts[None, :],
        quad_weight.reshape(-1, LANES),
        spectral_gain,
        channel_mix,
    )


def solution(mesh):
    return jax.shard_map(
        body,
        mesh=mesh,
        in_specs=(P(("group", "lat"), None, None), P(), P(), P("lat", None, None), P(), P(), P()),
        out_specs=P(("group", "lat"), None, None),
        check_vma=False,
    )
```
